32 devices in a mesh: seq: 8 (over z, x), tp: 4 (over y, core).
Axes of the slice: x: 2, y: 2, z: 4, core: 2. Of those that a mesh axis runs over, the one named last changes fastest.
Arguments:
- layer_in: bfloat16 [6144, 2048], P('seq', 'tp'), may hold values from -6 to 6
- attn_gain: float32 [2048], replicated, may hold values from 0.1 to 1.9
- qkv_weight: bfloat16 [3, 2048, 1024], P(None, None, 'tp'), may hold values from -0.125 to 0.125
- log_decay: float32 [8, 6144], P('tp', 'seq'), may hold values from -0.1 to 0
- write_rate: float32 [8, 6144], P('tp', 'seq'), may hold values from 0 to 0.9
- head_gain: float32 [128], replicated, may hold values from 0.1 to 1.9
- out_weight: bfloat16 [1024, 2048], P('tp'), may hold values from -0.1875 to 0.1875
- ffn_gain: float32 [2048], replicated, may hold values from 0.1 to 1.9
- gate_weight: bfloat16 [2048, 2560], P(None, 'tp'), may hold values from -0.125 to 0.125
- up_weight: bfloat16 [2048, 2560], P(None, 'tp'), may hold values from -0.125 to 0.125
- down_weight: bfloat16 [2560, 2048], P('tp'), may hold values from -0.125 to 0.125
Outputs:
- layer_out: bfloat16 [6144, 2048], P('seq', 'tp')
The draws below stay inside these ranges and needn't reach their ends.
All inputs are finite; a program needn't handle non-finite values.
Results may differ from the reference program's by a relative error of at most 0.014.
Values may be sent and summed in bfloat16 or wider, within the bound.
A program may use at most 128 MiB of HBM per device.

```python
import math
import jax
import jax.numpy as jnp
from jax import lax

D = 2048
HEADS = 8
DK = 128
FF = 2560
TOK_DEV = 768
SEQLEN = 6144
N_TP = 4


def head_kinds(key):
    kind_key = jax.random.fold_in(key, 101)
    order_key = jax.random.fold_in(key, 102)
    slow_share = 0.5
    slow_heads = jax.random.uniform(kind_key, (HEADS,)) < slow_share
    order = jax.random.permutation(order_key, HEADS)
    slow_heads = slow_heads.at[order[0]].set(True)
    slow_heads = slow_heads.at[order[1]].set(False)
    return slow_heads


def draw_log_decay(key, part):
    slow_heads = head_kinds(key)
    slow_rate = jax.random.uniform(jax.random.fold_in(key, 1), (HEADS, 1), minval=0.2, maxval=0.6) / SEQLEN
    fast_rate = jax.random.uniform(jax.random.fold_in(key, 2), (HEADS, 1), minval=1.0 / 50.0, maxval=1.0 / 30.0)
    base_rate = jnp.where(slow_heads[:, None], slow_rate, fast_rate)
    blocks = SEQLEN // TOK_DEV
    device_scale = jnp.exp(jax.random.uniform(jax.random.fold_in(key, 3), (HEADS, blocks, 1), minval=math.log(0.5), maxval=math.log(2.0)))
    device_scale = jnp.broadcast_to(device_scale, (HEADS, blocks, TOK_DEV)).reshape(HEADS, SEQLEN)
    jitter = jax.random.uniform(jax.random.fold_in(key, 4), (HEADS, SEQLEN), minval=0.5, maxval=1.5)
    return -(base_rate * device_scale * jitter).astype(jnp.float32)


def draw_write_rate(key, part):
    slow_heads = head_kinds(key)
    slow_rate = jax.random.uniform(jax.random.fold_in(key, 5), (HEADS, SEQLEN), minval=0.05, maxval=0.4) * DK / SEQLEN
    fast_rate = jax.random.uniform(jax.random.fold_in(key, 6), (HEADS, SEQLEN), minval=0.1, maxval=0.9)
    chosen = jnp.where(slow_heads[:, None], slow_rate, fast_rate)
    return jnp.minimum(chosen, 0.9).astype(jnp.float32)


def level_of(rng, extent, shards, low, largest):
    factor_of = 1.0
    for axis_at, blocks in shards:
        heights = jax.random.uniform(jax.random.fold_in(jax.random.fold_in(rng, 6), axis_at), (blocks,), jnp.float32, low / len(shards), largest / len(shards))
        factor_of = factor_of * jnp.repeat(jnp.exp(heights), extent[axis_at] // blocks).reshape((-1,) + (1,) * (len(extent) - 1 - axis_at))
    return factor_of


def gaussian(own_key, shape, spread, bound, shards=(), held_as=jnp.bfloat16):
    drawn = jax.random.normal(own_key, shape, jnp.float32) * spread
    if len(shards) > 0:
        drawn = level_of(own_key, shape, shards, -0.22, 0.18) * drawn
    return jnp.clip(drawn, min=-bound, max=bound).astype(held_as)


def setup_inputs(seed: int = 0) -> dict:
    key_of = jax.random.split(jax.random.key(seed), 12)
    return {
        "layer_in": gaussian(key_of[0], (SEQLEN, D), 1.0, 6.0, ((0, 8), (1, 4))),
        "attn_gain": jnp.clip(1.0 + 0.18 * jax.random.normal(key_of[1], (D,), jnp.float32), 0.1, 1.9),
        "qkv_weight": gaussian(key_of[2], (3, D, HEADS * DK), D ** -0.5, 0.125, ((2, 4),)),
        "log_decay": draw_log_decay(jax.random.fold_in(key_of[11], 71), 0),
        "write_rate": draw_write_rate(jax.random.fold_in(key_of[11], 71), 0),
        "head_gain": jnp.clip(1.0 + 0.18 * jax.random.normal(key_of[5], (DK,), jnp.float32), 0.1, 1.9),
        "out_weight": gaussian(key_of[6], (HEADS * DK, D), (HEADS * DK) ** -0.5, 0.1875, ((0, 4),)),
        "ffn_gain": jnp.clip(1.0 + 0.18 * jax.random.normal(key_of[7], (D,), jnp.float32), 0.1, 1.9),
        "gate_weight": gaussian(key_of[8], (D, FF), D ** -0.5, 0.125, ((1, 4),)),
        "up_weight": gaussian(key_of[9], (D, FF), D ** -0.5, 0.125, ((1, 4),)),
        "down_weight": gaussian(key_of[10], (FF, D), FF ** -0.5, 0.125, ((0, 4),)),
    }


norm_floor = 0.1
head_floor = 0.05

def rms_scale(values, gain, floor):
    return values * lax.rsqrt(lax.optimization_barrier(jnp.mean(values * values, axis=-1, keepdims=True)) + floor) * gain

def unit_rows(vectors):
    return vectors * lax.rsqrt(lax.optimization_barrier(jnp.sum(vectors * vectors, axis=-1, keepdims=True)) + 1.0)

def grouped_sum(left_side, right_side, groups):
    group_span = right_side.shape[0] // groups
    running = jnp.zeros((left_side.shape[0], right_side.shape[1]), jnp.float32)
    for member in range(groups):
        partial_value = jnp.dot(left_side[:, member * group_span:(member + 1) * group_span], right_side[member * group_span:(member + 1) * group_span], preferred_element_type=jnp.float32)
        running = running + partial_value.astype(jnp.bfloat16).astype(jnp.float32)
    return running

def token_step(memory, inputs):
    queries, key_rows, values, decay_step, write_step = inputs
    projected = lax.optimization_barrier(jnp.sum(key_rows[:, :, None] * memory, axis=1))
    memory = decay_step[:, None, None] * (memory - write_step[:, None, None] * key_rows[:, :, None] * projected[:, None, :]) + write_step[:, None, None] * key_rows[:, :, None] * values[:, None, :]
    output = lax.optimization_barrier(jnp.sum(queries[:, :, None] * memory, axis=1))
    return (memory, output)

def reference(layer_in, attn_gain, qkv_weight, log_decay, write_rate, head_gain, out_weight, ffn_gain, gate_weight, up_weight, down_weight):
    inputs = layer_in.astype(jnp.float32)
    normed = rms_scale(inputs, attn_gain, norm_floor).astype(jnp.bfloat16)
    queries = jnp.dot(normed, qkv_weight[0], preferred_element_type=jnp.float32).reshape(SEQLEN, HEADS, DK)
    key_rows = jnp.dot(normed, qkv_weight[1], preferred_element_type=jnp.float32).reshape(SEQLEN, HEADS, DK)
    values = jnp.dot(normed, qkv_weight[2], preferred_element_type=jnp.float32).reshape(SEQLEN, HEADS, DK)
    queries = unit_rows(queries)
    key_rows = unit_rows(key_rows)
    start = jnp.zeros((HEADS, DK, DK), jnp.float32)
    final_memory, heads_raw = lax.scan(token_step, start, (queries, key_rows, values, jnp.exp(log_decay).T, write_rate.T))
    heads_out = rms_scale(heads_raw, head_gain, head_floor).reshape(SEQLEN, HEADS * DK).astype(jnp.bfloat16)
    attn = grouped_sum(heads_out, out_weight, N_TP)
    residual = inputs + attn
    normed_mid = rms_scale(residual, ffn_gain, norm_floor).astype(jnp.bfloat16)
    gate_act = jnp.dot(normed_mid, gate_weight, preferred_element_type=jnp.float32)
    up_act = jnp.dot(normed_mid, up_weight, preferred_element_type=jnp.float32)
    hidden = (jax.nn.silu(gate_act) * up_act).astype(jnp.bfloat16)
    ffn = grouped_sum(hidden, down_weight, N_TP)
    return (residual + ffn).astype(jnp.bfloat16)
```

```python
import functools

import jax
import jax.numpy as jnp
from jax import lax
from jax.experimental import pallas as pl
from jax.experimental.pallas import tpu as pltpu
from jax.sharding import PartitionSpec as P

norm_floor = 0.1
head_floor = 0.05
bf16 = jnp.bfloat16
f32 = jnp.float32
MESH = pl.DeviceIdType.MESH
SPAN = 2
VL = 59
EARLY = (0, 1, 1, 2)
EARLY_TWIN = (2, 3, 3, 3)


def mm(a, b):
    return jnp.dot(a, b, preferred_element_type=f32)


def mm_nt(a, b):
    return lax.dot_general(a, b, (((1,), (1,)), ((), ())), preferred_element_type=f32)


def mm_tn(a, b):
    return lax.dot_general(a, b, (((0,), (0,)), ((), ())), preferred_element_type=f32)


def split_mm(a, b):
    high = a.astype(bf16)
    low = (a - high.astype(f32)).astype(bf16)
    return mm(high, b) + mm(low, b)


def unit_rows(u):
    return u * lax.rsqrt(jnp.sum(u * u, axis=-1, keepdims=True) + 1.0)


def kernel(
    cfg,
    x_hbm,
    again_ref,
    qkv_hbm,
    decay_ref,
    rate_ref,
    hgain_ref,
    wo_hbm,
    fgain_ref,
    gate_hbm,
    up_hbm,
    down_hbm,
    out_ref,
    x_full,
    qkv_w,
    gate_w,
    up_w,
    down_w,
    wo_full,
    o_buf,
    p_buf,
    heads_all,
    state,
    excl,
    s_send_buf,
    s_recv_buf,
    last_send_buf,
    last_recv_buf,
    res_tmp,
    res_own,
    part_buf,
    rp_buf,
    cs_buf,
    cr_buf,
    l_sem,
    x_send,
    x_recv,
    w_send,
    w_recv,
    f_send,
    f_recv,
    q_send,
    q_recv,
    b_send,
    b_recv,
    h_send,
    h_recv,
    s_send,
    s_recv,
    rp_send,
    rp_recv,
    rc_send,
    rc_recv,
):
    n_tp, n_seq, span, width, steps, group, nb = cfg
    length, cw = x_hbm.shape
    heads = qkv_hbm.shape[2] // width
    hw = heads * width
    half = n_tp // 2
    nc = length // span
    piece = width
    nh = length // piece
    share = hw // group
    sub = share // nb
    subs = span // width
    t = lax.axis_index("tp")
    s = lax.axis_index("seq")
    pt = t + 1 - 2 * lax.rem(t, 2)
    r = lax.rem(s, group)
    twin = s + 1 - 2 * r

    def to_tp(k):
        return lax.rem(t + 2 * k, n_tp)

    def from_tp(k):
        return lax.rem(t + n_tp - 2 * k, n_tp)

    def pair_tp(k):
        return lax.rem(pt + n_tp - 2 * k, n_tp)

    barrier = pltpu.get_barrier_semaphore()
    arrivals = 0
    for other in [pt] + [to_tp(k) for k in range(1, half)] + [from_tp(k) for k in range(1, half)]:
        pl.semaphore_signal(barrier, inc=1, device_id={"tp": other}, device_id_type=MESH)
        arrivals += 1
    for j in range(steps):
        d = 2**j

        @pl.when(s + d < n_seq)
        def _(d=d):
            pl.semaphore_signal(barrier, inc=1, device_id={"seq": s + d}, device_id_type=MESH)

        @pl.when(s >= d)
        def _(d=d):
            pl.semaphore_signal(barrier, inc=1, device_id={"seq": s - d}, device_id_type=MESH)

        arrivals = arrivals + 1 - (s + d) // n_seq + (s + n_seq - d) // n_seq

    def cols(j, w):
        return pl.ds(pl.multiple_of(j * w, w), w)

    def rows(i):
        return pl.ds(pl.multiple_of(i * span, span), span)

    def fine(i):
        return pl.ds(pl.multiple_of(i * piece, piece), piece)

    loads = [
        pltpu.make_async_copy(x_hbm, x_full.at[:, cols(t, cw)], l_sem.at[1]),
        pltpu.make_async_copy(qkv_hbm, qkv_w, l_sem.at[0]),
        pltpu.make_async_copy(wo_hbm, wo_full.at[cols(t, hw), :], l_sem.at[2]),
        pltpu.make_async_copy(gate_hbm, gate_w, l_sem.at[3]),
        pltpu.make_async_copy(up_hbm, up_w, l_sem.at[4]),
        pltpu.make_async_copy(down_hbm, down_w, l_sem.at[5]),
    ]
    for load in loads[:2]:
        load.start()
    pl.semaphore_wait(barrier, arrivals)
    loads[0].wait()

    def remote(src, dst, send, recv, axis, other):
        return pltpu.make_async_remote_copy(
            src_ref=src,
            dst_ref=dst,
            send_sem=send,
            recv_sem=recv,
            device_id={axis: other},
            device_id_type=MESH,
        )

    def x_slot(i, who):
        return x_full.at[rows(i), cols(who, cw)]

    def x_copy(slot, i, src, who, other):
        return remote(src, x_slot(i, who), x_send.at[slot, i], x_recv.at[slot, i], "tp", other)

    def h_slot(i, who):
        return heads_all.at[fine(i), cols(who, hw)]

    def h_copy(slot, i, who, other):
        return remote(
            h_slot(i, who), h_slot(i, who), h_send.at[slot, i], h_recv.at[slot, i], "tp", other
        )

    def w_slot(who):
        return wo_full.at[cols(who, hw), :]

    def w_rows(k, j, b):
        start = from_tp(k) * hw + j * share + b * sub
        return wo_full.at[pl.ds(pl.multiple_of(start, sub), sub), :]

    def pair_rows(k, j, b):
        start = pair_tp(k) * hw + j * share + b * sub
        return wo_full.at[pl.ds(pl.multiple_of(start, sub), sub), :]

    def far_copy(k, b):
        src = wo_hbm.at[pl.ds(pl.multiple_of(r * share + b * sub, sub), sub), :]
        dst = wo_full.at[pl.ds(pl.multiple_of(t * hw + r * share + b * sub, sub), sub), :]
        return remote(src, dst, f_send.at[k - 1, b], f_recv.at[k - 1, b], "tp", to_tp(k))

    def twin_copy(k, b):
        slot = w_rows(k, r, b)
        return remote(slot, slot, q_send.at[k - 1, b], q_recv.at[k - 1, b], "seq", twin)

    def pass_copy(k, g, j, b):
        slot = w_rows(k, j, b)
        return remote(slot, slot, b_send.at[k - 1, g, b], b_recv.at[k - 1, g, b], "tp", pt)

    def spread(b):
        for k in range(1, half):
            far_copy(k, b).wait_recv()
            if group > 1:
                twin_copy(k, b).start()
            pass_copy(k, 0, r, b).start()

    def spread_twin(b):
        for k in range(1, half):
            if group > 1:
                twin_copy(k, b).wait_recv()
                pass_copy(k, 1, 1 - r, b).start()

    def w_copy(slot, src, who, other):
        return remote(src, w_slot(who), w_send.at[slot], w_recv.at[slot], "tp", other)

    def send_x(i, carry):
        for k in range(1, half):
            x_copy(k, i, x_slot(i, t), t, to_tp(k)).start()
        x_copy(0, i, x_slot(i, t), t, pt).start()
        return carry

    lax.fori_loop(0, nc, send_x, 0)
    for load in loads[2:]:
        load.start()
    loads[1].wait()

    row_id = lax.broadcasted_iota(jnp.int32, (width, width), 0)
    col_id = lax.broadcasted_iota(jnp.int32, (width, width), 1)
    eye = (row_id == col_id).astype(f32)
    upto = (row_id <= col_id).astype(f32)
    for h in range(heads):
        state[h] = jnp.concatenate([eye, jnp.zeros((width, width), f32)], axis=1)

    def stage_one(i, carry):
        for k in range(1, half):
            x_copy(k, i, x_slot(i, from_tp(k)), from_tp(k), pt).wait_recv()
            x_copy(half - 1 + k, i, x_slot(i, from_tp(k)), from_tp(k), pt).start()

        @pl.when(i == 1)
        def _():
            w_copy(0, wo_hbm, t, pt).start()

        @pl.when(i == nc - 2)
        def _():
            for b in range(nb):
                for k in range(1, half):
                    far_copy(k, b).start()

        x_copy(0, i, x_slot(i, pt), pt, pt).wait_recv()
        for k in range(1, half):
            x_copy(half - 1 + k, i, x_slot(i, pair_tp(k)), pair_tp(k), pt).wait_recv()
        x = x_full[rows(i), :].astype(f32)
        scale = lax.rsqrt(jnp.mean(x * x, axis=1, keepdims=True) + norm_floor)
        normed = (x * scale * again_ref[...]).astype(bf16)
        q_all = mm(normed, qkv_w[0])
        k_all = mm(normed, qkv_w[1])
        v_all = mm(normed, qkv_w[2])
        xor = row_id ^ col_id
        chains = [(c, h) for c in range(subs) for h in range(heads)]
        lower, mixing, right, tail, growth_q, last = {}, {}, {}, {}, {}, {}
        for c in range(subs):
            at = pl.ds(pl.multiple_of(i * span + c * width, width), width)
            cumul = jnp.dot(
                decay_ref[:, at], upto, precision=lax.Precision.HIGHEST, preferred_element_type=f32
            )
            rate = rate_ref[:, at]
            for h in range(heads):
                cell = (c, h)
                part = (slice(c * width, (c + 1) * width), slice(h * width, (h + 1) * width))
                q = unit_rows(q_all[part])
                k = unit_rows(k_all[part])
                v = v_all[part]
                c_row = jnp.broadcast_to(cumul[h : h + 1, :], (width, width))
                c_col = c_row.T
                b_col = jnp.broadcast_to(rate[h : h + 1, :], (width, width)).T
                c_end = cumul[h : h + 1, width - 1 : width]
                weights = jnp.exp(jnp.minimum(c_col - c_row, 0.0))
                growth = jnp.exp(c_col)
                kb = k.astype(bf16)
                both = mm_nt(jnp.concatenate([kb, q.astype(bf16)], axis=0), kb)
                lower[cell] = jnp.where(row_id > col_id, b_col * both[:width] * weights, 0.0)
                mixing[cell] = jnp.where(row_id >= col_id, both[width:] * weights, 0.0).astype(bf16)
                right[cell] = jnp.concatenate([b_col * v, b_col * growth * k], axis=1).astype(bf16)
                tail[cell] = (k * jnp.exp(c_end - c_col)).astype(bf16)
                growth_q[cell] = growth * q
                last[cell] = jnp.exp(c_end)
        inverse = {cell: eye - jnp.where(xor < 2, lower[cell], 0.0) for cell in chains}
        block = 2
        while block < width:
            now = (xor >= block) & (xor < 2 * block)
            small = {cell: inverse[cell].astype(bf16) for cell in chains}
            half_way = {
                cell: mm(small[cell], jnp.where(now, lower[cell], 0.0).astype(bf16))
                for cell in chains
            }
            inverse = {
                cell: inverse[cell] - mm(half_way[cell].astype(bf16), small[cell])
                for cell in chains
            }
            block *= 2
        solved = {cell: mm(inverse[cell].astype(bf16), right[cell]).astype(bf16) for cell in chains}
        mixed = {cell: mm(mixing[cell], solved[cell]) for cell in chains}
        moved = {cell: mm_tn(tail[cell], solved[cell]) for cell in chains}
        for c in range(subs):
            at = pl.ds(pl.multiple_of(i * span + c * width, width), width)
            for h in range(heads):
                cell = (c, h)
                lanes = slice(h * width, (h + 1) * width)
                before = state[h]
                before_b = before.astype(bf16)
                entry = (growth_q[cell] - mixed[cell][:, width:]).astype(bf16)
                entered = mm(entry, before_b)
                p_buf[at, lanes] = entered[:, :width].astype(bf16)
                o_buf[at, lanes] = mixed[cell][:, :width] + entered[:, width:]
                change = mm(moved[cell][:, width:].astype(bf16), before_b)
                after = last[cell] * before - change
                state[h] = jnp.concatenate(
                    [after[:, :width], after[:, width:] + moved[cell][:, :width]], axis=1
                )
        return carry

    lax.fori_loop(0, nc, stage_one, 0)

    def s_copy(j, h):
        src, dst = (s_send_buf.at[j, h], s_recv_buf.at[j, h])
        if j + 1 == steps:
            src, dst = (last_send_buf.at[h], last_recv_buf.at[h])
        return remote(src, dst, s_send.at[j, h], s_recv.at[j, h], "seq", lax.rem(s + 2**j, n_seq))

    def s_start(j, h):
        @pl.when(s + 2**j < n_seq)
        def _():
            if j + 1 == steps:
                last_send_buf[h] = state[h, :, width:].astype(bf16)
            else:
                s_send_buf[j, h] = state[h].astype(bf16)
            s_copy(j, h).start()

    early = [[] for _ in range(steps)]
    early_twin = [[] for _ in range(steps)]
    for b, j in enumerate(EARLY[:nb]):
        if j < steps:
            early[j].append(b)
    for b, j in enumerate(EARLY_TWIN[:nb]):
        if j < steps:
            early_twin[j].append(b)

    for h in range(heads):
        excl[h] = jnp.concatenate([eye, jnp.zeros((width, width), f32)], axis=1)
        if steps > 0:
            s_start(0, h)
    for j in range(steps):
        for b in early[j]:
            spread(b)
        for b in early_twin[j]:
            spread_twin(b)
        for h in range(heads):

            @pl.when(s >= 2**j)
            def _(j=j, h=h):
                s_copy(j, h).wait_recv()
                if j + 1 == steps:
                    mine = excl[h]
                    got = last_recv_buf[h]
                    excl[h, :, width:] = split_mm(mine[:, :width], got) + mine[:, width:]
                    return
                got = s_recv_buf[j, h]
                mine = state[h]
                new = split_mm(mine[:, :width], got)
                state[h] = jnp.concatenate(
                    [new[:, :width], new[:, width:] + mine[:, width:]], axis=1
                )

            if j + 1 < steps:
                s_start(j + 1, h)

                @pl.when(s >= 2**j)
                def _(j=j, h=h):
                    got = s_recv_buf[j, h]
                    if j == 0:
                        excl[h] = got.astype(f32)
                        return
                    mine = excl[h]
                    new = split_mm(mine[:, :width], got)
                    excl[h] = jnp.concatenate(
                        [new[:, :width], new[:, width:] + mine[:, width:]], axis=1
                    )

    def stage_two(i, carry):
        for h in range(heads):
            lanes = slice(h * width, (h + 1) * width)
            start = excl[h, :, width:].astype(bf16)
            raw = o_buf[fine(i), lanes] + mm(p_buf[fine(i), lanes], start)
            scale = lax.rsqrt(jnp.mean(raw * raw, axis=1, keepdims=True) + head_floor)
            place = pl.ds(pl.multiple_of(t * hw + h * width, width), width)
            heads_all[fine(i), place] = (raw * scale * hgain_ref[...]).astype(bf16)
        for k in range(1, half):
            h_copy(k, i, t, to_tp(k)).start()
        h_copy(0, i, t, pt).start()
        return carry

    lax.fori_loop(0, nh, stage_two, 0)
    for b in range(nb):
        if not any(b in some for some in early):
            spread(b)
    for b in range(nb):
        if not any(b in some for some in early_twin):
            spread_twin(b)
    for load in loads[2:]:
        load.wait()
    def relay_heads(i, carry):
        for k in range(1, half):
            h_copy(k, i, from_tp(k), pt).wait_recv()
            h_copy(half - 1 + k, i, from_tp(k), pt).start()
        return carry

    def rp_copy(slot, i, who):
        return remote(
            part_buf.at[fine(i), cols(who, cw)],
            rp_buf.at[slot, fine(i), :],
            rp_send.at[slot, i],
            rp_recv.at[slot, i],
            "tp",
            pt,
        )

    def rc_copy(k, i):
        return remote(
            cs_buf.at[k - 1, fine(i), :],
            cr_buf.at[k - 1, fine(i), :],
            rc_send.at[k - 1, i],
            rc_recv.at[k - 1, i],
            "tp",
            to_tp(k),
        )

    def pair_reduce(i):
        for k in range(1, half):
            rp_copy(k, i, pt).wait_recv()
            mine = part_buf[fine(i), cols(to_tp(k), cw)].astype(f32)
            cs_buf[k - 1, fine(i), :] = (mine + rp_buf[k, fine(i), :].astype(f32)).astype(bf16)
            rc_copy(k, i).start()

    relay_heads(0, 0)
    w_copy(0, w_slot(pt), pt, pt).wait_recv()
    for k in range(1, half):
        for b in range(nb):
            for g in range(group):
                slot = pair_rows(k, r + g * (1 - 2 * r), b)
                remote(
                    slot, slot, b_send.at[k - 1, g, b], b_recv.at[k - 1, g, b], "tp", pt
                ).wait_recv()

    def stage_three(i, carry):
        h_copy(0, i, pt, pt).wait_recv()
        for k in range(1, half):
            h_copy(half - 1 + k, i, pair_tp(k), pt).wait_recv()
        res = x_full[fine(i), :].astype(f32) + mm(heads_all[fine(i), :], wo_full[...])
        res_tmp[...] = res

        @pl.when(i + 1 < nh)
        def _():
            relay_heads(i + 1, 0)

        @pl.when(i > 0)
        def _():
            pair_reduce(i - 1)

        res = res_tmp[...]
        scale = lax.rsqrt(jnp.mean(res * res, axis=1, keepdims=True) + norm_floor)
        normed = (res * scale * fgain_ref[...]).astype(bf16)
        gate = mm(normed, gate_w[...])
        up = mm(normed, up_w[...])
        hidden = (gate / (1.0 + jnp.exp(-gate)) * up).astype(bf16)
        part_buf[fine(i), :] = mm(hidden, down_w[...]).astype(bf16)
        for k in range(1, half):
            rp_copy(k, i, lax.rem(pt + 2 * k, n_tp)).start()
        rp_copy(0, i, pt).start()
        res_own[fine(i), :] = res_tmp[:, cols(t, cw)]

        return carry

    lax.fori_loop(0, nh, stage_three, 0)
    pair_reduce(nh - 1)

    def finish(i, carry):
        rp_copy(0, i, pt).wait_recv()
        total = res_own[fine(i), :] + part_buf[fine(i), cols(t, cw)].astype(f32)
        total = total + rp_buf[0, fine(i), :].astype(f32)
        for k in range(1, half):
            rc_copy(k, i).wait_recv()
            total = total + cr_buf[k - 1, fine(i), :].astype(f32)
        out_ref[fine(i), :] = total.astype(bf16)
        return carry

    lax.fori_loop(0, nh, finish, 0)

    def drain(i, carry):
        for k in range(1, half):
            x_copy(k, i, x_slot(i, t), t, to_tp(k)).wait_send()
            x_copy(half - 1 + k, i, x_slot(i, from_tp(k)), from_tp(k), pt).wait_send()
        x_copy(0, i, x_slot(i, t), t, pt).wait_send()
        return carry

    def drain_fine(i, carry):
        for k in range(1, half):
            h_copy(k, i, t, to_tp(k)).wait_send()
            h_copy(half - 1 + k, i, from_tp(k), pt).wait_send()
            rp_copy(k, i, lax.rem(pt + 2 * k, n_tp)).wait_send()
            rc_copy(k, i).wait_send()
        h_copy(0, i, t, pt).wait_send()
        rp_copy(0, i, pt).wait_send()
        return carry

    lax.fori_loop(0, nc, drain, 0)
    lax.fori_loop(0, nh, drain_fine, 0)
    for k in range(1, half):
        for b in range(nb):
            far_copy(k, b).wait_send()
            if group > 1:
                twin_copy(k, b).wait_send()
            for g in range(group):
                pass_copy(k, g, r + g * (1 - 2 * r), b).wait_send()
    w_copy(0, wo_hbm, t, pt).wait_send()
    for j in range(steps):

        @pl.when(s + 2**j < n_seq)
        def _(j=j):
            for h in range(heads):
                s_copy(j, h).wait_send()


def body(n_tp, n_seq, x, again, qkv, decay, rate, hgain, wo, fgain, gate, up, down):
    length, cw = x.shape
    width = hgain.shape[0]
    heads = qkv.shape[2] // width
    hw = heads * width
    full = cw * n_tp
    half = n_tp // 2
    span = SPAN * width
    nc = length // span
    steps = (n_seq - 1).bit_length()
    slots = 2 * half - 1
    nh = length // width
    group = 2 if n_seq % 2 == 0 else 1
    nb = 4
    anywhere = pl.BlockSpec(memory_space=pl.ANY)
    vmem = pl.BlockSpec(memory_space=pltpu.VMEM)
    dma = pltpu.SemaphoreType.DMA
    return pl.pallas_call(
        functools.partial(kernel, (n_tp, n_seq, span, width, steps, group, nb)),
        out_shape=pltpu.VMEM((length, cw), bf16),
        in_specs=[
            anywhere,
            vmem,
            anywhere,
            vmem,
            vmem,
            vmem,
            anywhere,
            vmem,
            anywhere,
            anywhere,
            anywhere,
        ],
        out_specs=pl.BlockSpec(memory_space=pltpu.VMEM),
        scratch_shapes=[
            pltpu.VMEM((length, full), bf16),
            pltpu.VMEM(qkv.shape, bf16),
            pltpu.VMEM(gate.shape, bf16),
            pltpu.VMEM(up.shape, bf16),
            pltpu.VMEM(down.shape, bf16),
            pltpu.VMEM((hw * n_tp, full), bf16),
            pltpu.VMEM((length, hw), f32),
            pltpu.VMEM((length, hw), bf16),
            pltpu.VMEM((length, hw * n_tp), bf16),
            pltpu.VMEM((heads, width, 2 * width), f32),
            pltpu.VMEM((heads, width, 2 * width), f32),
            pltpu.VMEM((steps, heads, width, 2 * width), bf16),
            pltpu.VMEM((steps, heads, width, 2 * width), bf16),
            pltpu.VMEM((heads, width, width), bf16),
            pltpu.VMEM((heads, width, width), bf16),
            pltpu.VMEM((width, full), f32),
            pltpu.VMEM((length, cw), f32),
            pltpu.VMEM((length, full), bf16),
            pltpu.VMEM((half, length, cw), bf16),
            pltpu.VMEM((half - 1, length, cw), bf16),
            pltpu.VMEM((half - 1, length, cw), bf16),
            dma((6,)),
            dma((slots, nc)),
            dma((slots, nc)),
            dma((1,)),
            dma((1,)),
            dma((half - 1, nb)),
            dma((half - 1, nb)),
            dma((half - 1, nb)),
            dma((half - 1, nb)),
            dma((half - 1, group, nb)),
            dma((half - 1, group, nb)),
            dma((slots, nh)),
            dma((slots, nh)),
            dma((steps, heads)),
            dma((steps, heads)),
            dma((half, nh)),
            dma((half, nh)),
            dma((half - 1, nh)),
            dma((half - 1, nh)),
        ],
        compiler_params=pltpu.CompilerParams(
            collective_id=0, has_side_effects=True, vmem_limit_bytes=VL * 1024 * 1024
        ),
    )(
        x,
        again.reshape(1, full),
        qkv,
        decay,
        rate,
        hgain.reshape(1, width),
        wo,
        fgain.reshape(1, full),
        gate,
        up,
        down,
    )


def solution(mesh):
    placed = (
        P("seq", "tp"),
        P(),
        P(None, None, "tp"),
        P("tp", "seq"),
        P("tp", "seq"),
        P(),
        P("tp", None),
        P(),
        P(None, "tp"),
        P(None, "tp"),
        P("tp", None),
    )
    return jax.shard_map(
        functools.partial(body, mesh.shape["tp"], mesh.shape["seq"]),
        mesh=mesh,
        in_specs=placed,
        out_specs=P("seq", "tp"),
        check_vma=False,
    )
```

```python
import functools

import jax
import jax.numpy as jnp
from jax import lax
from jax.experimental import pallas as pl
from jax.experimental.pallas import tpu as pltpu
from jax.sharding import PartitionSpec as P

norm_floor = 0.1
head_floor = 0.05
bf16 = jnp.bfloat16
f32 = jnp.float32
MESH = pl.DeviceIdType.MESH
VL = 59
XG = 1
FAR = 2
EARLY = (0, 1, 2, 2)
EARLY_TWIN = (2, 3, 3, 3)


def mm(a, b):
    return jnp.dot(a, b, preferred_element_type=f32)


def mm_nt(a, b):
    return lax.dot_general(a, b, (((1,), (1,)), ((), ())), preferred_element_type=f32)


def mm_tn(a, b):
    return lax.dot_general(a, b, (((0,), (0,)), ((), ())), preferred_element_type=f32)


def split_mm(a, b):
    high = a.astype(bf16)
    low = (a - high.astype(f32)).astype(bf16)
    return mm(high, b) + mm(low, b)


def unit_rows(u):
    return u * lax.rsqrt(jnp.sum(u * u, axis=-1, keepdims=True) + 1.0)


def kernel(
    cfg,
    x_hbm,
    again_hbm,
    qkv_hbm,
    decay_hbm,
    rate_hbm,
    hgain_hbm,
    wo_hbm,
    fgain_hbm,
    gate_hbm,
    up_hbm,
    down_hbm,
    out_ref,
    again_ref,
    decay_ref,
    rate_ref,
    hgain_ref,
    fgain_ref,
    below_buf,
    upto_buf,
    rate_buf,
    growth_buf,
    grown_buf,
    tail_buf,
    last_buf,
    x_full,
    qkv_w,
    gate_w,
    up_w,
    down_w,
    wo_full,
    o_buf,
    p_buf,
    heads_all,
    state,
    excl,
    s_send_buf,
    s_recv_buf,
    last_send_buf,
    last_recv_buf,
    heads_own,
    res_tmp,
    base_buf,
    pair_buf,
    part_buf,
    cr_buf,
    l_sem,
    x_send,
    x_recv,
    w_send,
    w_recv,
    f_send,
    f_recv,
    q_send,
    q_recv,
    b_send,
    b_recv,
    h_send,
    h_recv,
    s_send,
    s_recv,
    e_send,
    e_recv,
    rp_send,
    rp_recv,
    rc_send,
    rc_recv,
):
    n_tp, n_seq, span, width, steps, group, nb = cfg
    length, cw = x_hbm.shape
    full = cw * n_tp
    parts = 4
    heads = qkv_hbm.shape[2] // width
    hw = heads * width
    half = n_tp // 2
    nc = length // span
    piece = width
    nh = length // piece
    mine = nh // 2
    hidden_w = gate_hbm.shape[1]
    share = hw // group
    sub = share // nb
    t = lax.axis_index("tp")
    s = lax.axis_index("seq")
    c = lax.rem(t, 2)
    chip = t // 2
    pt = t + 1 - 2 * c
    r = lax.rem(s, group)
    twin = s + 1 - 2 * r

    def to_tp(k):
        return lax.rem(t + 2 * k, n_tp)

    def from_tp(k):
        return lax.rem(t + n_tp - 2 * k, n_tp)

    def pair_tp(k):
        return lax.rem(pt + n_tp - 2 * k, n_tp)

    def cross(k, e):
        return lax.rem(chip + k, half) * 2 + e

    def crossed(k, e):
        return lax.rem(chip + half - k, half) * 2 + e

    barrier = pltpu.get_barrier_semaphore()
    arrivals = 0
    for other in [pt] + [cross(k, e) for k in range(1, half) for e in range(2)]:
        pl.semaphore_signal(barrier, inc=1, device_id={"tp": other}, device_id_type=MESH)
        arrivals += 1
    for j in range(steps):
        d = 2**j

        @pl.when(s + d < n_seq)
        def _(d=d):
            pl.semaphore_signal(barrier, inc=1, device_id={"seq": s + d}, device_id_type=MESH)

        @pl.when(s >= d)
        def _(d=d):
            pl.semaphore_signal(barrier, inc=1, device_id={"seq": s - d}, device_id_type=MESH)

        arrivals = arrivals + 1 - (s + d) // n_seq + (s + n_seq - d) // n_seq

    def cols(j, w):
        return pl.ds(pl.multiple_of(j * w, w), w)

    def rows(i):
        return pl.ds(pl.multiple_of(i * span, span), span)

    def fine(i):
        return pl.ds(pl.multiple_of(i * piece, piece), piece)

    loads = [
        pltpu.make_async_copy(x_hbm, x_full.at[:, cols(t, cw)], l_sem.at[1]),
        pltpu.make_async_copy(qkv_hbm, qkv_w, l_sem.at[0]),
        pltpu.make_async_copy(wo_hbm, wo_full.at[cols(t, hw), :], l_sem.at[2]),
        pltpu.make_async_copy(gate_hbm, gate_w.at[:, cols(c, hidden_w)], l_sem.at[3]),
        pltpu.make_async_copy(up_hbm, up_w.at[:, cols(c, hidden_w)], l_sem.at[4]),
        pltpu.make_async_copy(down_hbm, down_w.at[cols(c, hidden_w), :], l_sem.at[5]),
    ]
    small = [
        pltpu.make_async_copy(src, dst, l_sem.at[6 + n])
        for n, (src, dst) in enumerate(
            (
                (again_hbm, again_ref),
                (decay_hbm, decay_ref),
                (rate_hbm, rate_ref),
                (hgain_hbm, hgain_ref),
                (fgain_hbm, fgain_ref),
            )
        )
    ]
    loads[0].start()
    for load in small:
        load.start()
    loads[1].start()
    pl.semaphore_wait(barrier, arrivals)
    loads[0].wait()

    def remote(src, dst, send, recv, axis, other):
        return pltpu.make_async_remote_copy(
            src_ref=src,
            dst_ref=dst,
            send_sem=send,
            recv_sem=recv,
            device_id={axis: other},
            device_id_type=MESH,
        )

    def x_slot(i, who):
        return x_full.at[rows(i), cols(who, cw)]

    def x_copy(slot, i, src, who, other):
        return remote(src, x_slot(i, who), x_send.at[slot, i], x_recv.at[slot, i], "tp", other)

    def h_slot(i, who):
        return heads_all.at[fine(i), cols(who, hw)]

    def h_copy(k, i):
        e = lax.rem(i, 2)
        slot, other = (0, pt) if k == 0 else (1 + (k - 1) * 2 + c, cross(k, e))
        return remote(
            heads_own.at[fine(i), :],
            h_slot(i // 2, t),
            h_send.at[k, i],
            h_recv.at[slot, i // 2],
            "tp",
            other,
        )

    def h_wait(i):
        for k in range(half):
            for e in range(2 if k > 0 else 1):
                who, slot = (pt, 0) if k == 0 else (crossed(k, e), 1 + (k - 1) * 2 + e)
                remote(
                    heads_own.at[fine(i), :],
                    h_slot(i, who),
                    h_send.at[k, i],
                    h_recv.at[slot, i],
                    "tp",
                    who,
                ).wait_recv()

    def e_copy(n, i, who):
        if n == 2:
            size = hidden_w // parts
            at = pl.ds(pl.multiple_of(i * size, size), size)
            dst = down_w.at[pl.ds(pl.multiple_of(who * hidden_w + i * size, size), size), :]
            src = down_hbm.at[at, :]
        else:
            size = full // parts
            at = pl.ds(pl.multiple_of(i * size, size), size)
            dst = (gate_w, up_w)[n].at[at, cols(who, hidden_w)]
            src = (gate_hbm, up_hbm)[n].at[at, :]
        return remote(src, dst, e_send.at[n, i], e_recv.at[n, i], "tp", pt)

    def share_weights(first, stop):
        for i in range(first, stop):
            for n in range(3):
                e_copy(n, i, c).start()

    def w_slot(who):
        return wo_full.at[cols(who, hw), :]

    def w_rows(k, j, b):
        start = from_tp(k) * hw + j * share + b * sub
        return wo_full.at[pl.ds(pl.multiple_of(start, sub), sub), :]

    def pair_rows(k, j, b):
        start = pair_tp(k) * hw + j * share + b * sub
        return wo_full.at[pl.ds(pl.multiple_of(start, sub), sub), :]

    def far_copy(k, b):
        src = wo_hbm.at[pl.ds(pl.multiple_of(r * share + b * sub, sub), sub), :]
        dst = wo_full.at[pl.ds(pl.multiple_of(t * hw + r * share + b * sub, sub), sub), :]
        return remote(src, dst, f_send.at[k - 1, b], f_recv.at[k - 1, b], "tp", to_tp(k))

    def twin_copy(k, b):
        slot = w_rows(k, r, b)
        return remote(slot, slot, q_send.at[k - 1, b], q_recv.at[k - 1, b], "seq", twin)

    def pass_copy(k, g, j, b):
        slot = w_rows(k, j, b)
        return remote(slot, slot, b_send.at[k - 1, g, b], b_recv.at[k - 1, g, b], "tp", pt)

    def spread(b):
        for k in range(1, half):
            far_copy(k, b).wait_recv()
            if group > 1:
                twin_copy(k, b).start()
            pass_copy(k, 0, r, b).start()

    def spread_twin(b):
        for k in range(1, half):
            if group > 1:
                twin_copy(k, b).wait_recv()
                pass_copy(k, 1, 1 - r, b).start()

    def w_copy(slot, src, who, other):
        return remote(src, w_slot(who), w_send.at[slot], w_recv.at[slot], "tp", other)

    def send_x(i, carry):
        for k in range(1, half):
            x_copy(k, i, x_slot(i, t), t, to_tp(k)).start()
        x_copy(0, i, x_slot(i, t), t, pt).start()
        return carry

    lax.fori_loop(0, nc, send_x, 0)
    for load in loads[2:]:
        load.start()
    w_copy(0, wo_hbm, t, pt).start()
    share_weights(0, parts // 2)
    for load in small:
        load.wait()

    row_id = lax.broadcasted_iota(jnp.int32, (width, width), 0)
    col_id = lax.broadcasted_iota(jnp.int32, (width, width), 1)
    eye = (row_id == col_id).astype(f32)
    upto = (row_id <= col_id).astype(f32)
    for h in range(heads):
        state[h] = jnp.concatenate([eye, jnp.zeros((width, width), f32)], axis=1)

    xor = row_id ^ col_id

    def fold_gain(i, carry):
        at = cols(i, width)
        gain = jnp.broadcast_to(again_ref[:, at], (width, width)).T
        gain = jnp.concatenate([gain] * heads, axis=1)
        for j in range(3):
            qkv_w[j, at, :] = (qkv_w[j, at, :].astype(f32) * gain).astype(bf16)
        return carry

    def prepare(i, carry):
        at = fine(i)
        lanes = cols(i, width)
        cumul = jnp.dot(
            decay_ref[:, lanes], upto, precision=lax.Precision.HIGHEST, preferred_element_type=f32
        )
        rate = rate_ref[:, lanes]
        for h in range(heads):
            c_row = jnp.broadcast_to(cumul[h : h + 1, :], (width, width))
            c_col = c_row.T
            b_col = jnp.broadcast_to(rate[h : h + 1, :], (width, width)).T
            c_end = cumul[h : h + 1, width - 1 : width]
            weights = jnp.exp(jnp.minimum(c_col - c_row, 0.0))
            growth = jnp.exp(c_col)
            below_buf[h, at, :] = jnp.where(row_id > col_id, b_col * weights, 0.0)
            upto_buf[h, at, :] = jnp.where(row_id >= col_id, weights, 0.0)
            rate_buf[h, at, :] = b_col
            growth_buf[h, at, :] = growth
            grown_buf[h, at, :] = b_col * growth
            tail_buf[h, at, :] = jnp.exp(c_end - c_col)
            last_buf[i, h : h + 1, :] = jnp.broadcast_to(jnp.exp(c_end), (1, 2 * width))
        return carry

    lax.fori_loop(0, nh, prepare, 0)
    loads[1].wait()
    lax.fori_loop(0, full // width, fold_gain, 0)

    def gather(i):
        for k in range(1, half):
            x_copy(k, i, x_slot(i, from_tp(k)), from_tp(k), pt).wait_recv()
            x_copy(half - 1 + k, i, x_slot(i, from_tp(k)), from_tp(k), pt).start()

    def gathered(i):
        x_copy(0, i, x_slot(i, pt), pt, pt).wait_recv()
        for k in range(1, half):
            x_copy(half - 1 + k, i, x_slot(i, pair_tp(k)), pair_tp(k), pt).wait_recv()

    def invert(lower):
        chains = list(lower)
        inverse = {cell: eye - jnp.where(xor < 2, lower[cell], 0.0) for cell in chains}
        block = 2
        while block < width:
            merge = 4 if 4 * block <= width else 2
            now = (xor >= block) & (xor < merge * block)
            small = {cell: inverse[cell].astype(bf16) for cell in chains}
            off = {
                cell: mm(small[cell], jnp.where(now, lower[cell], 0.0).astype(bf16)).astype(bf16)
                for cell in chains
            }
            inverse = {cell: inverse[cell] - mm(off[cell], small[cell]) for cell in chains}
            if merge == 4:
                square = {cell: mm(off[cell], off[cell]).astype(bf16) for cell in chains}
                inverse = {
                    cell: inverse[cell] + mm(square[cell], inverse[cell].astype(bf16))
                    for cell in chains
                }
            block *= merge
        return inverse

    def chunk(first, subs, between=None):
        span = subs * width
        here = pl.ds(pl.multiple_of(first, width), span)
        x = x_full[here, :]
        wide = x.astype(f32)
        scale = lax.rsqrt(jnp.mean(wide * wide, axis=1, keepdims=True) + norm_floor)
        k_all = mm(x, qkv_w[1]) * scale
        v_all = mm(x, qkv_w[2]) * scale
        q_all = mm(x, qkv_w[0]) * scale
        chains = [(c, h) for c in range(subs) for h in range(heads)]
        lower, mixing, right, tail, growth_q, last = {}, {}, {}, {}, {}, {}
        for c in range(subs):
            at = pl.ds(pl.multiple_of(first + c * width, width), width)
            for h in range(heads):
                cell = (c, h)
                part = (slice(c * width, (c + 1) * width), slice(h * width, (h + 1) * width))
                q = unit_rows(q_all[part])
                k = unit_rows(k_all[part])
                kb = k.astype(bf16)
                both = mm_nt(jnp.concatenate([kb, q.astype(bf16)], axis=0), kb)
                lower[cell] = both[:width] * below_buf[h, at, :]
                mixing[cell] = (both[width:] * upto_buf[h, at, :]).astype(bf16)
                right[cell] = jnp.concatenate(
                    [rate_buf[h, at, :] * v_all[part], grown_buf[h, at, :] * k], axis=1
                ).astype(bf16)
                tail[cell] = (k * tail_buf[h, at, :]).astype(bf16)
                growth_q[cell] = growth_buf[h, at, :] * q
                last[cell] = last_buf[first // width + c, h : h + 1, :]
        inverse = invert(lower)
        solved = {cell: mm(inverse[cell].astype(bf16), right[cell]).astype(bf16) for cell in chains}
        moved = {cell: mm_tn(tail[cell], solved[cell]) for cell in chains}
        before_b = {}
        for c in range(subs):
            for h in range(heads):
                cell = (c, h)
                before = state[h]
                before_b[cell] = before.astype(bf16)
                change = mm(moved[cell][:, width:].astype(bf16), before_b[cell])
                after = last[cell] * before - change
                state[h] = jnp.concatenate(
                    [after[:, :width], after[:, width:] + moved[cell][:, :width]], axis=1
                )
        if between is not None:
            between()
        mixed = {cell: mm(mixing[cell], solved[cell]) for cell in chains}
        for c in range(subs):
            at = pl.ds(pl.multiple_of(first + c * width, width), width)
            for h in range(heads):
                cell = (c, h)
                lanes = slice(h * width, (h + 1) * width)
                entry = (growth_q[cell] - mixed[cell][:, width:]).astype(bf16)
                entered = mm(entry, before_b[cell])
                p_buf[at, lanes] = entered[:, :width].astype(bf16)
                o_buf[at, lanes] = mixed[cell][:, :width] + entered[:, width:]

    def s_copy(j, h):
        src, dst = (s_send_buf.at[j, h], s_recv_buf.at[j, h])
        if j + 1 == steps:
            src, dst = (last_send_buf.at[h], last_recv_buf.at[h])
        return remote(src, dst, s_send.at[j, h], s_recv.at[j, h], "seq", lax.rem(s + 2**j, n_seq))

    def s_start(j, h):
        @pl.when(s + 2**j < n_seq)
        def _():
            if j + 1 == steps:
                last_send_buf[h] = state[h, :, width:].astype(bf16)
            else:
                s_send_buf[j, h] = state[h].astype(bf16)
            s_copy(j, h).start()

    early = [[] for _ in range(steps)]
    early_twin = [[] for _ in range(steps)]
    for b, j in enumerate(EARLY[:nb]):
        if j < steps:
            early[j].append(b)
    for b, j in enumerate(EARLY_TWIN[:nb]):
        if j < steps:
            early_twin[j].append(b)

    subs = 2 if nh % 2 == 0 else 1
    per = subs * width // span
    big = nh // subs

    def stage_one(i, carry):
        for n in range(1, per):
            gather(per * i + n)

        @pl.when(i == FAR)
        def _():
            for b in range(nb):
                for k in range(1, half):
                    far_copy(k, b).start()
            share_weights(parts // 2, parts)

        for n in range(per):
            gathered(per * i + n)

        def between():
            @pl.when(i + 1 < big)
            def _():
                gather(per * (i + 1))

            @pl.when(i + 1 == big)
            def _():
                for h in range(heads):
                    excl[h] = jnp.concatenate([eye, jnp.zeros((width, width), f32)], axis=1)
                    if steps > 0:
                        s_start(0, h)

        chunk(i * subs * width, subs, between)
        return carry

    gather(0)
    lax.fori_loop(0, big, stage_one, 0)
    for j in range(steps):
        for b in early[j]:
            spread(b)
        for b in early_twin[j]:
            spread_twin(b)
        for h in range(heads):

            @pl.when(s >= 2**j)
            def _(j=j, h=h):
                s_copy(j, h).wait_recv()
                if j + 1 == steps:
                    mine = excl[h]
                    got = last_recv_buf[h]
                    excl[h, :, width:] = split_mm(mine[:, :width], got) + mine[:, width:]
                    return
                got = s_recv_buf[j, h]
                mine = state[h]
                new = split_mm(mine[:, :width], got)
                state[h] = jnp.concatenate(
                    [new[:, :width], new[:, width:] + mine[:, width:]], axis=1
                )

            if j + 1 < steps:
                s_start(j + 1, h)

                @pl.when(s >= 2**j)
                def _(j=j, h=h):
                    got = s_recv_buf[j, h]
                    if j == 0:
                        excl[h] = got.astype(f32)
                        return
                    mine = excl[h]
                    new = split_mm(mine[:, :width], got)
                    excl[h] = jnp.concatenate(
                        [new[:, :width], new[:, width:] + mine[:, width:]], axis=1
                    )

    def stage_two(i, carry):
        for h in range(heads):
            lanes = slice(h * width, (h + 1) * width)
            start = excl[h, :, width:].astype(bf16)
            raw = o_buf[fine(i), lanes] + mm(p_buf[fine(i), lanes], start)
            scale = lax.rsqrt(jnp.mean(raw * raw, axis=1, keepdims=True) + head_floor)
            heads_own[fine(i), lanes] = (raw * scale * hgain_ref[...]).astype(bf16)
        for k in range(1, half):
            h_copy(k, i).start()

        @pl.when(lax.rem(i, 2) != c)
        def _():
            h_copy(0, i).start()

        @pl.when(lax.rem(i, 2) == c)
        def _():
            heads_all[fine(i // 2), cols(t, hw)] = heads_own[fine(i), :]

        return carry

    lax.fori_loop(0, nh, stage_two, 0)
    for b in range(nb):
        if not any(b in some for some in early):
            spread(b)
    for b in range(nb):
        if not any(b in some for some in early_twin):
            spread_twin(b)
    for load in loads[2:]:
        load.wait()
    for i in range(parts):
        for n in range(3):
            e_copy(n, i, 1 - c).wait_recv()

    def base_copy(i):
        return remote(
            pair_buf.at[fine(i), :],
            base_buf.at[fine(2 * i + c), :],
            rp_send.at[i],
            rp_recv.at[i],
            "tp",
            pt,
        )

    def rc_copy(k, e, i):
        p = 2 * i + c
        return remote(
            part_buf.at[fine(i), cols(cross(k, e), cw)],
            cr_buf.at[k - 1, fine(p), :],
            rc_send.at[k - 1, e, i],
            rc_recv.at[k - 1, p],
            "tp",
            cross(k, e),
        )

    w_copy(0, w_slot(pt), pt, pt).wait_recv()
    for k in range(1, half):
        for b in range(nb):
            for g in range(group):
                slot = pair_rows(k, r + g * (1 - 2 * r), b)
                remote(
                    slot, slot, b_send.at[k - 1, g, b], b_recv.at[k - 1, g, b], "tp", pt
                ).wait_recv()

    def stage_three(i, carry):
        p = 2 * i + c
        h_wait(i)
        res = x_full[fine(p), :].astype(f32) + mm(heads_all[fine(i), :], wo_full[...])
        scale = lax.rsqrt(jnp.mean(res * res, axis=1, keepdims=True) + norm_floor)
        res_tmp[...] = res
        normed = (res * scale * fgain_ref[...]).astype(bf16)
        gate = mm(normed, gate_w[...])
        up = mm(normed, up_w[...])
        hidden = (gate / (1.0 + jnp.exp(-gate)) * up).astype(bf16)
        part = mm(hidden, down_w[...])
        part_buf[fine(i), :] = part.astype(bf16)
        for k in range(1, half):
            for e in range(2):
                rc_copy(k, e, i).start()
        res_tmp[...] = res_tmp[...] + part
        pair_buf[fine(i), :] = res_tmp[:, cols(pt, cw)]
        base_copy(i).start()
        base_buf[fine(p), :] = res_tmp[:, cols(t, cw)]
        return carry

    lax.fori_loop(0, mine, stage_three, 0)

    def finish(p, carry):
        @pl.when(lax.rem(p, 2) != c)
        def _():
            remote(
                pair_buf.at[fine(p // 2), :],
                base_buf.at[fine(p), :],
                rp_send.at[p // 2],
                rp_recv.at[p // 2],
                "tp",
                pt,
            ).wait_recv()

        total = base_buf[fine(p), :]
        for k in range(1, half):
            remote(
                part_buf.at[fine(p // 2), cols(t, cw)],
                cr_buf.at[k - 1, fine(p), :],
                rc_send.at[k - 1, 0, p // 2],
                rc_recv.at[k - 1, p],
                "tp",
                crossed(k, lax.rem(p, 2)),
            ).wait_recv()
            total = total + cr_buf[k - 1, fine(p), :].astype(f32)
        out_ref[fine(p), :] = total.astype(bf16)
        return carry

    lax.fori_loop(0, nh, finish, 0)

    def drain(i, carry):
        for k in range(1, half):
            x_copy(k, i, x_slot(i, t), t, to_tp(k)).wait_send()
            x_copy(half - 1 + k, i, x_slot(i, from_tp(k)), from_tp(k), pt).wait_send()
        x_copy(0, i, x_slot(i, t), t, pt).wait_send()
        return carry

    def drain_heads(i, carry):
        for k in range(1, half):
            h_copy(k, i).wait_send()

        @pl.when(lax.rem(i, 2) != c)
        def _():
            h_copy(0, i).wait_send()

        return carry

    def drain_fine(i, carry):
        for k in range(1, half):
            for e in range(2):
                rc_copy(k, e, i).wait_send()
        base_copy(i).wait_send()
        return carry

    lax.fori_loop(0, nc, drain, 0)
    lax.fori_loop(0, nh, drain_heads, 0)
    lax.fori_loop(0, mine, drain_fine, 0)
    for i in range(parts):
        for n in range(3):
            e_copy(n, i, c).wait_send()
    for k in range(1, half):
        for b in range(nb):
            far_copy(k, b).wait_send()
            if group > 1:
                twin_copy(k, b).wait_send()
            for g in range(group):
                pass_copy(k, g, r + g * (1 - 2 * r), b).wait_send()
    w_copy(0, wo_hbm, t, pt).wait_send()
    for j in range(steps):

        @pl.when(s + 2**j < n_seq)
        def _(j=j):
            for h in range(heads):
                s_copy(j, h).wait_send()


def body(n_tp, n_seq, x, again, qkv, decay, rate, hgain, wo, fgain, gate, up, down):
    length, cw = x.shape
    width = hgain.shape[0]
    heads = qkv.shape[2] // width
    hw = heads * width
    full = cw * n_tp
    parts = 4
    half = n_tp // 2
    span = XG * width
    nc = length // span
    steps = (n_seq - 1).bit_length()
    slots = 2 * half - 1
    nh = length // width
    group = 2 if n_seq % 2 == 0 else 1
    nb = 4
    anywhere = pl.BlockSpec(memory_space=pl.ANY)
    dma = pltpu.SemaphoreType.DMA
    return pl.pallas_call(
        functools.partial(kernel, (n_tp, n_seq, span, width, steps, group, nb)),
        out_shape=pltpu.VMEM((length, cw), bf16),
        in_specs=[anywhere] * 11,
        out_specs=pl.BlockSpec(memory_space=pltpu.VMEM),
        scratch_shapes=[
            pltpu.VMEM((1, full), f32),
            pltpu.VMEM(decay.shape, f32),
            pltpu.VMEM(rate.shape, f32),
            pltpu.VMEM((1, width), f32),
            pltpu.VMEM((1, full), f32),
            *[pltpu.VMEM((heads, length, width), f32)] * 6,
            pltpu.VMEM((nh, heads, 2 * width), f32),
            pltpu.VMEM((length, full), bf16),
            pltpu.VMEM(qkv.shape, bf16),
            pltpu.VMEM((full, 2 * gate.shape[1]), bf16),
            pltpu.VMEM((full, 2 * up.shape[1]), bf16),
            pltpu.VMEM((2 * down.shape[0], full), bf16),
            pltpu.VMEM((hw * n_tp, full), bf16),
            pltpu.VMEM((length, hw), f32),
            pltpu.VMEM((length, hw), bf16),
            pltpu.VMEM((length // 2, hw * n_tp), bf16),
            pltpu.VMEM((heads, width, 2 * width), f32),
            pltpu.VMEM((heads, width, 2 * width), f32),
            pltpu.VMEM((steps, heads, width, 2 * width), bf16),
            pltpu.VMEM((steps, heads, width, 2 * width), bf16),
            pltpu.VMEM((heads, width, width), bf16),
            pltpu.VMEM((heads, width, width), bf16),
            pltpu.VMEM((length, hw), bf16),
            pltpu.VMEM((width, full), f32),
            pltpu.VMEM((length, cw), f32),
            pltpu.VMEM((length // 2, cw), f32),
            pltpu.VMEM((length // 2, full), bf16),
            pltpu.VMEM((half - 1, length, cw), bf16),
            dma((11,)),
            dma((slots, nc)),
            dma((slots, nc)),
            dma((1,)),
            dma((1,)),
            dma((half - 1, nb)),
            dma((half - 1, nb)),
            dma((half - 1, nb)),
            dma((half - 1, nb)),
            dma((half - 1, group, nb)),
            dma((half - 1, group, nb)),
            dma((half, nh)),
            dma((slots, nh // 2)),
            dma((steps, heads)),
            dma((steps, heads)),
            dma((3, parts)),
            dma((3, parts)),
            dma((nh // 2,)),
            dma((nh // 2,)),
            dma((half - 1, 2, nh // 2)),
            dma((half - 1, nh)),
        ],
        compiler_params=pltpu.CompilerParams(
            collective_id=0, has_side_effects=True, vmem_limit_bytes=VL * 1024 * 1024
        ),
    )(
        x,
        again.reshape(1, full),
        qkv,
        decay,
        rate,
        hgain.reshape(1, width),
        wo,
        fgain.reshape(1, full),
        gate,
        up,
        down,
    )


def solution(mesh):
    placed = (
        P("seq", "tp"),
        P(),
        P(None, None, "tp"),
        P("tp", "seq"),
        P("tp", "seq"),
        P(),
        P("tp", None),
        P(),
        P(None, "tp"),
        P(None, "tp"),
        P("tp", None),
    )
    return jax.shard_map(
        functools.partial(body, mesh.shape["tp"], mesh.shape["seq"]),
        mesh=mesh,
        in_specs=placed,
        out_specs=P("seq", "tp"),
        check_vma=False,
    )
```

```python
import functools

import jax
import jax.numpy as jnp
from jax import lax
from jax.experimental import pallas as pl
from jax.experimental.pallas import tpu as pltpu
from jax.sharding import PartitionSpec as P

norm_floor = 0.1
head_floor = 0.05
bf16 = jnp.bfloat16
f32 = jnp.float32
MESH = pl.DeviceIdType.MESH
VL = 59
XG = 1
FAR = 2
EARLY = (0, 1, 2, 2)
EARLY_TWIN = (2, 2, 3, 3)


def mm(a, b):
    return jnp.dot(a, b, preferred_element_type=f32)


def mm_nt(a, b):
    return lax.dot_general(a, b, (((1,), (1,)), ((), ())), preferred_element_type=f32)


def mm_tn(a, b):
    return lax.dot_general(a, b, (((0,), (0,)), ((), ())), preferred_element_type=f32)


def split_mm(a, b):
    high = a.astype(bf16)
    low = (a - high.astype(f32)).astype(bf16)
    return mm(high, b) + mm(low, b)


def unit_rows(u):
    return u * lax.rsqrt(jnp.sum(u * u, axis=-1, keepdims=True) + 1.0)


def kernel(
    cfg,
    x_hbm,
    again_hbm,
    qkv_hbm,
    decay_hbm,
    rate_hbm,
    hgain_hbm,
    wo_hbm,
    fgain_hbm,
    gate_hbm,
    up_hbm,
    down_hbm,
    out_ref,
    again_ref,
    decay_ref,
    rate_ref,
    hgain_ref,
    fgain_ref,
    below_buf,
    upto_buf,
    rate_buf,
    growth_buf,
    grown_buf,
    tail_buf,
    last_buf,
    early_buf,
    square_buf,
    x_full,
    qkv_w,
    gate_w,
    up_w,
    down_w,
    wo_full,
    o_buf,
    p_buf,
    heads_all,
    state,
    excl,
    s_send_buf,
    s_recv_buf,
    last_send_buf,
    last_recv_buf,
    heads_own,
    res_tmp,
    base_buf,
    pair_buf,
    part_buf,
    cr_buf,
    l_sem,
    x_send,
    x_recv,
    w_send,
    w_recv,
    f_send,
    f_recv,
    q_send,
    q_recv,
    b_send,
    b_recv,
    h_send,
    h_recv,
    s_send,
    s_recv,
    e_send,
    e_recv,
    rp_send,
    rp_recv,
    rc_send,
    rc_recv,
):
    n_tp, n_seq, span, width, steps, group, nb = cfg
    length, cw = x_hbm.shape
    full = cw * n_tp
    parts = 4
    heads = qkv_hbm.shape[2] // width
    hw = heads * width
    half = n_tp // 2
    nc = length // span
    piece = width
    nh = length // piece
    mine = nh // 2
    hidden_w = gate_hbm.shape[1]
    share = hw // group
    sub = share // nb
    t = lax.axis_index("tp")
    s = lax.axis_index("seq")
    c = lax.rem(t, 2)
    chip = t // 2
    pt = t + 1 - 2 * c
    r = lax.rem(s, group)
    twin = s + 1 - 2 * r

    def to_tp(k):
        return lax.rem(t + 2 * k, n_tp)

    def from_tp(k):
        return lax.rem(t + n_tp - 2 * k, n_tp)

    def pair_tp(k):
        return lax.rem(pt + n_tp - 2 * k, n_tp)

    def cross(k, e):
        return lax.rem(chip + k, half) * 2 + e

    def crossed(k, e):
        return lax.rem(chip + half - k, half) * 2 + e

    barrier = pltpu.get_barrier_semaphore()
    arrivals = 0
    for other in [pt] + [cross(k, e) for k in range(1, half) for e in range(2)]:
        pl.semaphore_signal(barrier, inc=1, device_id={"tp": other}, device_id_type=MESH)
        arrivals += 1
    for j in range(steps):
        d = 2**j

        @pl.when(s + d < n_seq)
        def _(d=d):
            pl.semaphore_signal(barrier, inc=1, device_id={"seq": s + d}, device_id_type=MESH)

        @pl.when(s >= d)
        def _(d=d):
            pl.semaphore_signal(barrier, inc=1, device_id={"seq": s - d}, device_id_type=MESH)

        arrivals = arrivals + 1 - (s + d) // n_seq + (s + n_seq - d) // n_seq

    def cols(j, w):
        return pl.ds(pl.multiple_of(j * w, w), w)

    def rows(i):
        return pl.ds(pl.multiple_of(i * span, span), span)

    def fine(i):
        return pl.ds(pl.multiple_of(i * piece, piece), piece)

    loads = [
        pltpu.make_async_copy(x_hbm, x_full.at[:, cols(t, cw)], l_sem.at[1]),
        pltpu.make_async_copy(qkv_hbm, qkv_w, l_sem.at[0]),
        pltpu.make_async_copy(wo_hbm, wo_full.at[cols(t, hw), :], l_sem.at[2]),
        pltpu.make_async_copy(gate_hbm, gate_w.at[:, cols(c, hidden_w)], l_sem.at[3]),
        pltpu.make_async_copy(up_hbm, up_w.at[:, cols(c, hidden_w)], l_sem.at[4]),
        pltpu.make_async_copy(down_hbm, down_w.at[cols(c, hidden_w), :], l_sem.at[5]),
    ]
    small = [
        pltpu.make_async_copy(src, dst, l_sem.at[6 + n])
        for n, (src, dst) in enumerate(
            (
                (again_hbm, again_ref),
                (decay_hbm, decay_ref),
                (rate_hbm, rate_ref),
                (hgain_hbm, hgain_ref),
                (fgain_hbm, fgain_ref),
            )
        )
    ]
    loads[0].start()
    for load in small:
        load.start()
    loads[1].start()
    pl.semaphore_wait(barrier, arrivals)
    loads[0].wait()

    def remote(src, dst, send, recv, axis, other):
        return pltpu.make_async_remote_copy(
            src_ref=src,
            dst_ref=dst,
            send_sem=send,
            recv_sem=recv,
            device_id={axis: other},
            device_id_type=MESH,
        )

    def x_slot(i, who):
        return x_full.at[rows(i), cols(who, cw)]

    def x_copy(slot, i, src, who, other):
        return remote(src, x_slot(i, who), x_send.at[slot, i], x_recv.at[slot, i], "tp", other)

    def h_slot(i, who):
        return heads_all.at[fine(i), cols(who, hw)]

    def h_copy(k, i):
        e = lax.rem(i, 2)
        slot, other = (0, pt) if k == 0 else (1 + (k - 1) * 2 + c, cross(k, e))
        return remote(
            heads_own.at[fine(i), :],
            h_slot(i // 2, t),
            h_send.at[k, i],
            h_recv.at[slot, i // 2],
            "tp",
            other,
        )

    def h_wait(i):
        for k in range(half):
            for e in range(2 if k > 0 else 1):
                who, slot = (pt, 0) if k == 0 else (crossed(k, e), 1 + (k - 1) * 2 + e)
                remote(
                    heads_own.at[fine(i), :],
                    h_slot(i, who),
                    h_send.at[k, i],
                    h_recv.at[slot, i],
                    "tp",
                    who,
                ).wait_recv()

    def e_copy(n, i, who):
        if n == 2:
            size = hidden_w // parts
            at = pl.ds(pl.multiple_of(i * size, size), size)
            dst = down_w.at[pl.ds(pl.multiple_of(who * hidden_w + i * size, size), size), :]
            src = down_hbm.at[at, :]
        else:
            size = full // parts
            at = pl.ds(pl.multiple_of(i * size, size), size)
            dst = (gate_w, up_w)[n].at[at, cols(who, hidden_w)]
            src = (gate_hbm, up_hbm)[n].at[at, :]
        return remote(src, dst, e_send.at[n, i], e_recv.at[n, i], "tp", pt)

    def share_weights(first, stop):
        for i in range(first, stop):
            for n in range(3):
                e_copy(n, i, c).start()

    def w_slot(who):
        return wo_full.at[cols(who, hw), :]

    def w_rows(k, j, b):
        start = from_tp(k) * hw + j * share + b * sub
        return wo_full.at[pl.ds(pl.multiple_of(start, sub), sub), :]

    def pair_rows(k, j, b):
        start = pair_tp(k) * hw + j * share + b * sub
        return wo_full.at[pl.ds(pl.multiple_of(start, sub), sub), :]

    def far_copy(k, b):
        src = wo_hbm.at[pl.ds(pl.multiple_of(r * share + b * sub, sub), sub), :]
        dst = wo_full.at[pl.ds(pl.multiple_of(t * hw + r * share + b * sub, sub), sub), :]
        return remote(src, dst, f_send.at[k - 1, b], f_recv.at[k - 1, b], "tp", to_tp(k))

    def twin_copy(k, b):
        slot = w_rows(k, r, b)
        return remote(slot, slot, q_send.at[k - 1, b], q_recv.at[k - 1, b], "seq", twin)

    def pass_copy(k, g, j, b):
        slot = w_rows(k, j, b)
        return remote(slot, slot, b_send.at[k - 1, g, b], b_recv.at[k - 1, g, b], "tp", pt)

    def spread(b):
        for k in range(1, half):
            far_copy(k, b).wait_recv()
            if group > 1:
                twin_copy(k, b).start()
            pass_copy(k, 0, r, b).start()

    def spread_twin(b):
        for k in range(1, half):
            if group > 1:
                twin_copy(k, b).wait_recv()
                pass_copy(k, 1, 1 - r, b).start()

    def w_copy(slot, src, who, other):
        return remote(src, w_slot(who), w_send.at[slot], w_recv.at[slot], "tp", other)

    def send_x(i, carry):
        for k in range(1, half):
            x_copy(k, i, x_slot(i, t), t, to_tp(k)).start()
        x_copy(0, i, x_slot(i, t), t, pt).start()
        return carry

    lax.fori_loop(0, nc, send_x, 0)
    for load in loads[2:]:
        load.start()
    w_copy(0, wo_hbm, t, pt).start()
    share_weights(0, parts // 2)
    for load in small:
        load.wait()

    row_id = lax.broadcasted_iota(jnp.int32, (width, width), 0)
    col_id = lax.broadcasted_iota(jnp.int32, (width, width), 1)
    eye = (row_id == col_id).astype(f32)
    upto = (row_id <= col_id).astype(f32)
    for h in range(heads):
        state[h] = jnp.concatenate([eye, jnp.zeros((width, width), f32)], axis=1)

    xor = row_id ^ col_id

    def fold_gain(i, carry):
        at = cols(i, width)
        gain = jnp.broadcast_to(again_ref[:, at], (width, width)).T
        gain = jnp.concatenate([gain] * heads, axis=1)
        for j in range(3):
            qkv_w[j, at, :] = (qkv_w[j, at, :].astype(f32) * gain).astype(bf16)
        return carry

    def prepare(i, carry):
        at = fine(i)
        lanes = cols(i, width)
        cumul = jnp.dot(
            decay_ref[:, lanes], upto, precision=lax.Precision.HIGHEST, preferred_element_type=f32
        )
        rate = rate_ref[:, lanes]
        for h in range(heads):
            c_row = jnp.broadcast_to(cumul[h : h + 1, :], (width, width))
            c_col = c_row.T
            b_col = jnp.broadcast_to(rate[h : h + 1, :], (width, width)).T
            c_end = cumul[h : h + 1, width - 1 : width]
            weights = jnp.exp(jnp.minimum(c_col - c_row, 0.0))
            growth = jnp.exp(c_col)
            below_buf[h, at, :] = jnp.where(row_id > col_id, b_col * weights, 0.0)
            upto_buf[h, at, :] = jnp.where(row_id >= col_id, weights, 0.0)
            rate_buf[h, at, :] = b_col
            growth_buf[h, at, :] = growth
            grown_buf[h, at, :] = b_col * growth
            tail_buf[h, at, :] = jnp.exp(c_end - c_col)
            last_buf[i, h : h + 1, :] = jnp.broadcast_to(jnp.exp(c_end), (1, 2 * width))
        return carry

    lax.fori_loop(0, nh, prepare, 0)
    loads[1].wait()
    lax.fori_loop(0, full // width, fold_gain, 0)

    def gather(i):
        for k in range(1, half):
            x_copy(k, i, x_slot(i, from_tp(k)), from_tp(k), pt).wait_recv()
            x_copy(half - 1 + k, i, x_slot(i, from_tp(k)), from_tp(k), pt).start()

    def gathered(i):
        for k in range(1, half):
            x_copy(half - 1 + k, i, x_slot(i, pair_tp(k)), pair_tp(k), pt).wait_recv()

    def solve(lower, right):
        chains = list(lower)
        inverse = {cell: eye - jnp.where(xor < 2, lower[cell], 0.0) for cell in chains}
        block = 2
        while block < width:
            merge = 4 if 4 * block <= width else 2
            now = (xor >= block) & (xor < merge * block)
            small = {cell: inverse[cell].astype(bf16) for cell in chains}
            off = {
                cell: mm(small[cell], jnp.where(now, lower[cell], 0.0).astype(bf16)).astype(bf16)
                for cell in chains
            }
            block *= merge
            if block == width:
                inverse = {cell: mm(small[cell], right[cell]) for cell in chains}
                small = {cell: inverse[cell].astype(bf16) for cell in chains}
            inverse = {cell: inverse[cell] - mm(off[cell], small[cell]) for cell in chains}
            if merge == 4:
                square = {cell: mm(off[cell], off[cell]).astype(bf16) for cell in chains}
                inverse = {
                    cell: inverse[cell] + mm(square[cell], inverse[cell].astype(bf16))
                    for cell in chains
                }
        return inverse

    def chunk(first, subs, between=None):
        span = subs * width
        here = pl.ds(pl.multiple_of(first, width), span)
        square = square_buf[here, :1]
        q_all, k_all, v_all = [early_buf[n, here, :] for n in range(3)]
        for n in range(1, half):
            at = cols(pair_tp(n), cw)
            x = x_full[here, at]
            wide = x.astype(f32)
            square = square + jnp.sum(wide * wide, axis=1, keepdims=True)
            k_all = k_all + mm(x, qkv_w[1, at, :])
            v_all = v_all + mm(x, qkv_w[2, at, :])
            q_all = q_all + mm(x, qkv_w[0, at, :])
        scale = lax.rsqrt(square * (1.0 / full) + norm_floor)
        q_all, k_all, v_all = q_all * scale, k_all * scale, v_all * scale
        chains = [(c, h) for c in range(subs) for h in range(heads)]
        lower, mixing, right, tail, growth_q, last = {}, {}, {}, {}, {}, {}
        for c in range(subs):
            at = pl.ds(pl.multiple_of(first + c * width, width), width)
            for h in range(heads):
                cell = (c, h)
                part = (slice(c * width, (c + 1) * width), slice(h * width, (h + 1) * width))
                q = unit_rows(q_all[part])
                k = unit_rows(k_all[part])
                kb = k.astype(bf16)
                both = mm_nt(jnp.concatenate([kb, q.astype(bf16)], axis=0), kb)
                lower[cell] = both[:width] * below_buf[h, at, :]
                mixing[cell] = (both[width:] * upto_buf[h, at, :]).astype(bf16)
                right[cell] = jnp.concatenate(
                    [rate_buf[h, at, :] * v_all[part], grown_buf[h, at, :] * k], axis=1
                ).astype(bf16)
                tail[cell] = (k * tail_buf[h, at, :]).astype(bf16)
                growth_q[cell] = growth_buf[h, at, :] * q
                last[cell] = last_buf[first // width + c, h : h + 1, :]
        answer = solve(lower, right)
        solved = {cell: answer[cell].astype(bf16) for cell in chains}
        moved = {cell: mm_tn(tail[cell], solved[cell]) for cell in chains}
        before_b = {}
        for c in range(subs):
            for h in range(heads):
                cell = (c, h)
                before = state[h]
                before_b[cell] = before.astype(bf16)
                change = mm(moved[cell][:, width:].astype(bf16), before_b[cell])
                after = last[cell] * before - change
                state[h] = jnp.concatenate(
                    [after[:, :width], after[:, width:] + moved[cell][:, :width]], axis=1
                )
        if between is not None:
            between()
        mixed = {cell: mm(mixing[cell], solved[cell]) for cell in chains}
        for c in range(subs):
            at = pl.ds(pl.multiple_of(first + c * width, width), width)
            for h in range(heads):
                cell = (c, h)
                lanes = slice(h * width, (h + 1) * width)
                entry = (growth_q[cell] - mixed[cell][:, width:]).astype(bf16)
                entered = mm(entry, before_b[cell])
                p_buf[at, lanes] = entered[:, :width].astype(bf16)
                o_buf[at, lanes] = mixed[cell][:, :width] + entered[:, width:]

    def s_copy(j, h):
        src, dst = (s_send_buf.at[j, h], s_recv_buf.at[j, h])
        if j + 1 == steps:
            src, dst = (last_send_buf.at[h], last_recv_buf.at[h])
        return remote(src, dst, s_send.at[j, h], s_recv.at[j, h], "seq", lax.rem(s + 2**j, n_seq))

    def s_start(j, h):
        @pl.when(s + 2**j < n_seq)
        def _():
            if j + 1 == steps:
                last_send_buf[h] = state[h, :, width:].astype(bf16)
            else:
                s_send_buf[j, h] = state[h].astype(bf16)
            s_copy(j, h).start()

    early = [[] for _ in range(steps)]
    early_twin = [[] for _ in range(steps)]
    for b, j in enumerate(EARLY[:nb]):
        if j < steps:
            early[j].append(b)
    for b, j in enumerate(EARLY_TWIN[:nb]):
        if j < steps:
            early_twin[j].append(b)

    subs = 2 if nh % 2 == 0 else 1
    per = subs * width // span
    big = nh // subs

    def stage_one(i, carry):
        for n in range(1, per):
            gather(per * i + n)

        @pl.when(i == FAR)
        def _():
            for b in range(nb):
                for k in range(1, half):
                    far_copy(k, b).start()
            share_weights(parts // 2, parts)

        here = pl.ds(pl.multiple_of(i * subs * width, subs * width), subs * width)
        for k in range(1, half):
            at = cols(from_tp(k), cw)
            x = x_full[here, at]
            wide = x.astype(f32)
            square_buf[here, :] += jnp.broadcast_to(
                jnp.sum(wide * wide, axis=1, keepdims=True), (subs * width, width)
            )
            for n in range(3):
                early_buf[n, here, :] += mm(x, qkv_w[n, at, :])
        for n in range(per):
            gathered(per * i + n)

        def between():
            @pl.when(i + 1 < big)
            def _():
                gather(per * (i + 1))

            @pl.when(i + 1 == big)
            def _():
                for h in range(heads):
                    excl[h] = jnp.concatenate([eye, jnp.zeros((width, width), f32)], axis=1)
                    if steps > 0:
                        s_start(0, h)

        chunk(i * subs * width, subs, between)
        return carry

    def stage_zero(i, carry):
        for n in range(per):
            x_copy(0, per * i + n, x_slot(per * i + n, pt), pt, pt).wait_recv()
        at = cols(chip, 2 * cw)
        here = pl.ds(pl.multiple_of(i * subs * width, subs * width), subs * width)
        x = x_full[here, at]
        wide = x.astype(f32)
        square = jnp.sum(wide * wide, axis=1, keepdims=True)
        square_buf[here, :] = jnp.broadcast_to(square, (subs * width, width))
        for n in range(3):
            early_buf[n, here, :] = mm(x, qkv_w[n, at, :])
        return carry

    lax.fori_loop(0, big, stage_zero, 0)
    gather(0)
    lax.fori_loop(0, big, stage_one, 0)
    for j in range(steps):
        for b in early[j]:
            spread(b)
        for b in early_twin[j]:
            spread_twin(b)
        for h in range(heads):

            @pl.when(s >= 2**j)
            def _(j=j, h=h):
                s_copy(j, h).wait_recv()
                if j + 1 == steps:
                    mine = excl[h]
                    got = last_recv_buf[h]
                    excl[h, :, width:] = split_mm(mine[:, :width], got) + mine[:, width:]
                    return
                got = s_recv_buf[j, h]
                mine = state[h]
                new = split_mm(mine[:, :width], got)
                state[h] = jnp.concatenate(
                    [new[:, :width], new[:, width:] + mine[:, width:]], axis=1
                )

            if j + 1 < steps:
                s_start(j + 1, h)

                @pl.when(s >= 2**j)
                def _(j=j, h=h):
                    got = s_recv_buf[j, h]
                    if j == 0:
                        excl[h] = got.astype(f32)
                        return
                    mine = excl[h]
                    new = split_mm(mine[:, :width], got)
                    excl[h] = jnp.concatenate(
                        [new[:, :width], new[:, width:] + mine[:, width:]], axis=1
                    )

    def stage_two(i, carry):
        for h in range(heads):
            lanes = slice(h * width, (h + 1) * width)
            start = excl[h, :, width:].astype(bf16)
            raw = o_buf[fine(i), lanes] + mm(p_buf[fine(i), lanes], start)
            scale = lax.rsqrt(jnp.mean(raw * raw, axis=1, keepdims=True) + head_floor)
            heads_own[fine(i), lanes] = (raw * scale * hgain_ref[...]).astype(bf16)
        for k in range(1, half):
            h_copy(k, i).start()

        @pl.when(lax.rem(i, 2) != c)
        def _():
            h_copy(0, i).start()

        @pl.when(lax.rem(i, 2) == c)
        def _():
            heads_all[fine(i // 2), cols(t, hw)] = heads_own[fine(i), :]

        return carry

    lax.fori_loop(0, nh, stage_two, 0)
    for b in range(nb):
        if not any(b in some for some in early):
            spread(b)
    for b in range(nb):
        if not any(b in some for some in early_twin):
            spread_twin(b)
    for load in loads[2:]:
        load.wait()
    for i in range(parts):
        for n in range(3):
            e_copy(n, i, 1 - c).wait_recv()

    def base_copy(i):
        return remote(
            pair_buf.at[fine(i), :],
            base_buf.at[fine(2 * i + c), :],
            rp_send.at[i],
            rp_recv.at[i],
            "tp",
            pt,
        )

    def rc_copy(k, e, i):
        p = 2 * i + c
        return remote(
            part_buf.at[fine(i), cols(cross(k, e), cw)],
            cr_buf.at[k - 1, fine(p), :],
            rc_send.at[k - 1, e, i],
            rc_recv.at[k - 1, p],
            "tp",
            cross(k, e),
        )

    w_copy(0, w_slot(pt), pt, pt).wait_recv()
    for k in range(1, half):
        for b in range(nb):
            for g in range(group):
                slot = pair_rows(k, r + g * (1 - 2 * r), b)
                remote(
                    slot, slot, b_send.at[k - 1, g, b], b_recv.at[k - 1, g, b], "tp", pt
                ).wait_recv()

    def stage_three(i, carry):
        p = 2 * i + c
        h_wait(i)
        res = x_full[fine(p), :].astype(f32) + mm(heads_all[fine(i), :], wo_full[...])
        scale = lax.rsqrt(jnp.mean(res * res, axis=1, keepdims=True) + norm_floor)
        res_tmp[...] = res
        normed = (res * scale * fgain_ref[...]).astype(bf16)
        gate = mm(normed, gate_w[...])
        up = mm(normed, up_w[...])
        hidden = (gate / (1.0 + jnp.exp(-gate)) * up).astype(bf16)
        part = mm(hidden, down_w[...])
        part_buf[fine(i), :] = part.astype(bf16)
        for k in range(1, half):
            for e in range(2):
                rc_copy(k, e, i).start()
        res_tmp[...] = res_tmp[...] + part
        pair_buf[fine(i), :] = res_tmp[:, cols(pt, cw)]
        base_copy(i).start()
        base_buf[fine(p), :] = res_tmp[:, cols(t, cw)]
        return carry

    lax.fori_loop(0, mine, stage_three, 0)

    def finish(p, carry):
        @pl.when(lax.rem(p, 2) != c)
        def _():
            remote(
                pair_buf.at[fine(p // 2), :],
                base_buf.at[fine(p), :],
                rp_send.at[p // 2],
                rp_recv.at[p // 2],
                "tp",
                pt,
            ).wait_recv()

        total = base_buf[fine(p), :]
        for k in range(1, half):
            remote(
                part_buf.at[fine(p // 2), cols(t, cw)],
                cr_buf.at[k - 1, fine(p), :],
                rc_send.at[k - 1, 0, p // 2],
                rc_recv.at[k - 1, p],
                "tp",
                crossed(k, lax.rem(p, 2)),
            ).wait_recv()
            total = total + cr_buf[k - 1, fine(p), :].astype(f32)
        out_ref[fine(p), :] = total.astype(bf16)
        return carry

    lax.fori_loop(0, nh, finish, 0)

    def drain(i, carry):
        for k in range(1, half):
            x_copy(k, i, x_slot(i, t), t, to_tp(k)).wait_send()
            x_copy(half - 1 + k, i, x_slot(i, from_tp(k)), from_tp(k), pt).wait_send()
        x_copy(0, i, x_slot(i, t), t, pt).wait_send()
        return carry

    def drain_heads(i, carry):
        for k in range(1, half):
            h_copy(k, i).wait_send()

        @pl.when(lax.rem(i, 2) != c)
        def _():
            h_copy(0, i).wait_send()

        return carry

    def drain_fine(i, carry):
        for k in range(1, half):
            for e in range(2):
                rc_copy(k, e, i).wait_send()
        base_copy(i).wait_send()
        return carry

    lax.fori_loop(0, nc, drain, 0)
    lax.fori_loop(0, nh, drain_heads, 0)
    lax.fori_loop(0, mine, drain_fine, 0)
    for i in range(parts):
        for n in range(3):
            e_copy(n, i, c).wait_send()
    for k in range(1, half):
        for b in range(nb):
            far_copy(k, b).wait_send()
            if group > 1:
                twin_copy(k, b).wait_send()
            for g in range(group):
                pass_copy(k, g, r + g * (1 - 2 * r), b).wait_send()
    w_copy(0, wo_hbm, t, pt).wait_send()
    for j in range(steps):

        @pl.when(s + 2**j < n_seq)
        def _(j=j):
            for h in range(heads):
                s_copy(j, h).wait_send()


def body(n_tp, n_seq, x, again, qkv, decay, rate, hgain, wo, fgain, gate, up, down):
    length, cw = x.shape
    width = hgain.shape[0]
    heads = qkv.shape[2] // width
    hw = heads * width
    full = cw * n_tp
    parts = 4
    half = n_tp // 2
    span = XG * width
    nc = length // span
    steps = (n_seq - 1).bit_length()
    slots = 2 * half - 1
    nh = length // width
    group = 2 if n_seq % 2 == 0 else 1
    nb = 4
    anywhere = pl.BlockSpec(memory_space=pl.ANY)
    dma = pltpu.SemaphoreType.DMA
    return pl.pallas_call(
        functools.partial(kernel, (n_tp, n_seq, span, width, steps, group, nb)),
        out_shape=pltpu.VMEM((length, cw), bf16),
        in_specs=[anywhere] * 11,
        out_specs=pl.BlockSpec(memory_space=pltpu.VMEM),
        scratch_shapes=[
            pltpu.VMEM((1, full), f32),
            pltpu.VMEM(decay.shape, f32),
            pltpu.VMEM(rate.shape, f32),
            pltpu.VMEM((1, width), f32),
            pltpu.VMEM((1, full), f32),
            *[pltpu.VMEM((heads, length, width), f32)] * 6,
            pltpu.VMEM((nh, heads, 2 * width), f32),
            pltpu.VMEM((3, length, hw), f32),
            pltpu.VMEM((length, width), f32),
            pltpu.VMEM((length, full), bf16),
            pltpu.VMEM(qkv.shape, bf16),
            pltpu.VMEM((full, 2 * gate.shape[1]), bf16),
            pltpu.VMEM((full, 2 * up.shape[1]), bf16),
            pltpu.VMEM((2 * down.shape[0], full), bf16),
            pltpu.VMEM((hw * n_tp, full), bf16),
            pltpu.VMEM((length, hw), f32),
            pltpu.VMEM((length, hw), bf16),
            pltpu.VMEM((length // 2, hw * n_tp), bf16),
            pltpu.VMEM((heads, width, 2 * width), f32),
            pltpu.VMEM((heads, width, 2 * width), f32),
            pltpu.VMEM((steps, heads, width, 2 * width), bf16),
            pltpu.VMEM((steps, heads, width, 2 * width), bf16),
            pltpu.VMEM((heads, width, width), bf16),
            pltpu.VMEM((heads, width, width), bf16),
            pltpu.VMEM((length, hw), bf16),
            pltpu.VMEM((width, full), f32),
            pltpu.VMEM((length, cw), f32),
            pltpu.VMEM((length // 2, cw), f32),
            pltpu.VMEM((length // 2, full), bf16),
            pltpu.VMEM((half - 1, length, cw), bf16),
            dma((11,)),
            dma((slots, nc)),
            dma((slots, nc)),
            dma((1,)),
            dma((1,)),
            dma((half - 1, nb)),
            dma((half - 1, nb)),
            dma((half - 1, nb)),
            dma((half - 1, nb)),
            dma((half - 1, group, nb)),
            dma((half - 1, group, nb)),
            dma((half, nh)),
            dma((slots, nh // 2)),
            dma((steps, heads)),
            dma((steps, heads)),
            dma((3, parts)),
            dma((3, parts)),
            dma((nh // 2,)),
            dma((nh // 2,)),
            dma((half - 1, 2, nh // 2)),
            dma((half - 1, nh)),
        ],
        compiler_params=pltpu.CompilerParams(
            collective_id=0, has_side_effects=True, vmem_limit_bytes=VL * 1024 * 1024
        ),
    )(
        x,
        again.reshape(1, full),
        qkv,
        decay,
        rate,
        hgain.reshape(1, width),
        wo,
        fgain.reshape(1, full),
        gate,
        up,
        down,
    )


def solution(mesh):
    placed = (
        P("seq", "tp"),
        P(),
        P(None, None, "tp"),
        P("tp", "seq"),
        P("tp", "seq"),
        P(),
        P("tp", None),
        P(),
        P(None, "tp"),
        P(None, "tp"),
        P("tp", None),
    )
    return jax.shard_map(
        functools.partial(body, mesh.shape["tp"], mesh.shape["seq"]),
        mesh=mesh,
        in_specs=placed,
        out_specs=P("seq", "tp"),
        check_vma=False,
    )
```

```python
import functools

import jax
import jax.numpy as jnp
from jax import lax
from jax.experimental import pallas as pl
from jax.experimental.pallas import tpu as pltpu
from jax.sharding import PartitionSpec as P

norm_floor = 0.1
head_floor = 0.05
bf16 = jnp.bfloat16
f32 = jnp.float32
MESH = pl.DeviceIdType.MESH
VL = 59
XG = 1
FAR = 2
EARLY = (0, 1, 2, 2)
EARLY_TWIN = (2, 2, 3, 3)


def mm(a, b):
    return jnp.dot(a, b, preferred_element_type=f32)


def mm_nt(a, b):
    return lax.dot_general(a, b, (((1,), (1,)), ((), ())), preferred_element_type=f32)


def mm_tn(a, b):
    return lax.dot_general(a, b, (((0,), (0,)), ((), ())), preferred_element_type=f32)


def split_mm(a, b):
    high = a.astype(bf16)
    low = (a - high.astype(f32)).astype(bf16)
    return mm(high, b) + mm(low, b)


def unit_rows(u):
    return u * lax.rsqrt(jnp.sum(u * u, axis=-1, keepdims=True) + 1.0)


def kernel(
    cfg,
    x_hbm,
    again_hbm,
    qkv_hbm,
    decay_hbm,
    rate_hbm,
    hgain_hbm,
    wo_hbm,
    fgain_hbm,
    gate_hbm,
    up_hbm,
    down_hbm,
    out_ref,
    again_ref,
    decay_ref,
    rate_ref,
    hgain_ref,
    fgain_ref,
    below_buf,
    upto_buf,
    rate_buf,
    growth_buf,
    grown_buf,
    tail_buf,
    last_buf,
    early_buf,
    square_buf,
    own_buf,
    x_full,
    qkv_w,
    gate_w,
    up_w,
    down_w,
    wo_full,
    o_buf,
    p_buf,
    heads_all,
    state,
    excl,
    s_send_buf,
    s_recv_buf,
    last_send_buf,
    last_recv_buf,
    heads_own,
    res_tmp,
    base_buf,
    pair_buf,
    part_buf,
    cr_buf,
    l_sem,
    x_send,
    x_recv,
    w_send,
    w_recv,
    f_send,
    f_recv,
    q_send,
    q_recv,
    b_send,
    b_recv,
    h_send,
    h_recv,
    s_send,
    s_recv,
    e_send,
    e_recv,
    rp_send,
    rp_recv,
    rc_send,
    rc_recv,
):
    n_tp, n_seq, span, width, steps, group, nb = cfg
    length, cw = x_hbm.shape
    full = cw * n_tp
    parts = 4
    heads = qkv_hbm.shape[2] // width
    hw = heads * width
    half = n_tp // 2
    nc = length // span
    piece = width
    nh = length // piece
    mine = nh // 2
    hidden_w = gate_hbm.shape[1]
    share = hw // group
    sub = share // nb
    t = lax.axis_index("tp")
    s = lax.axis_index("seq")
    c = lax.rem(t, 2)
    chip = t // 2
    pt = t + 1 - 2 * c
    r = lax.rem(s, group)
    twin = s + 1 - 2 * r

    def to_tp(k):
        return lax.rem(t + 2 * k, n_tp)

    def from_tp(k):
        return lax.rem(t + n_tp - 2 * k, n_tp)

    def pair_tp(k):
        return lax.rem(pt + n_tp - 2 * k, n_tp)

    def cross(k, e):
        return lax.rem(chip + k, half) * 2 + e

    def crossed(k, e):
        return lax.rem(chip + half - k, half) * 2 + e

    barrier = pltpu.get_barrier_semaphore()
    arrivals = 0
    for other in [pt] + [cross(k, e) for k in range(1, half) for e in range(2)]:
        pl.semaphore_signal(barrier, inc=1, device_id={"tp": other}, device_id_type=MESH)
        arrivals += 1
    for j in range(steps):
        d = 2**j

        @pl.when(s + d < n_seq)
        def _(d=d):
            pl.semaphore_signal(barrier, inc=1, device_id={"seq": s + d}, device_id_type=MESH)

        @pl.when(s >= d)
        def _(d=d):
            pl.semaphore_signal(barrier, inc=1, device_id={"seq": s - d}, device_id_type=MESH)

        arrivals = arrivals + 1 - (s + d) // n_seq + (s + n_seq - d) // n_seq

    def cols(j, w):
        return pl.ds(pl.multiple_of(j * w, w), w)

    def rows(i):
        return pl.ds(pl.multiple_of(i * span, span), span)

    def fine(i):
        return pl.ds(pl.multiple_of(i * piece, piece), piece)

    loads = [
        pltpu.make_async_copy(x_hbm, x_full.at[:, cols(t, cw)], l_sem.at[1]),
        pltpu.make_async_copy(qkv_hbm, qkv_w, l_sem.at[0]),
        pltpu.make_async_copy(wo_hbm, wo_full.at[cols(t, hw), :], l_sem.at[2]),
        pltpu.make_async_copy(gate_hbm, gate_w.at[:, cols(c, hidden_w)], l_sem.at[3]),
        pltpu.make_async_copy(up_hbm, up_w.at[:, cols(c, hidden_w)], l_sem.at[4]),
        pltpu.make_async_copy(down_hbm, down_w.at[cols(c, hidden_w), :], l_sem.at[5]),
    ]
    small = [
        pltpu.make_async_copy(src, dst, l_sem.at[6 + n])
        for n, (src, dst) in enumerate(
            (
                (again_hbm, again_ref),
                (decay_hbm, decay_ref),
                (rate_hbm, rate_ref),
                (hgain_hbm, hgain_ref),
                (fgain_hbm, fgain_ref),
            )
        )
    ]
    loads[0].start()
    for load in small:
        load.start()
    loads[1].start()
    pl.semaphore_wait(barrier, arrivals)
    loads[0].wait()

    def remote(src, dst, send, recv, axis, other):
        return pltpu.make_async_remote_copy(
            src_ref=src,
            dst_ref=dst,
            send_sem=send,
            recv_sem=recv,
            device_id={axis: other},
            device_id_type=MESH,
        )

    def x_slot(i, who):
        return x_full.at[rows(i), cols(who, cw)]

    def x_copy(slot, i, src, who, other):
        return remote(src, x_slot(i, who), x_send.at[slot, i], x_recv.at[slot, i], "tp", other)

    def h_slot(i, who):
        return heads_all.at[fine(i), cols(who, hw)]

    def h_copy(k, i):
        e = lax.rem(i, 2)
        slot, other = (0, pt) if k == 0 else (1 + (k - 1) * 2 + c, cross(k, e))
        return remote(
            heads_own.at[fine(i), :],
            h_slot(i // 2, t),
            h_send.at[k, i],
            h_recv.at[slot, i // 2],
            "tp",
            other,
        )

    def h_wait(i, some):
        for k in some:
            for e in range(2 if k > 0 else 1):
                who, slot = (pt, 0) if k == 0 else (crossed(k, e), 1 + (k - 1) * 2 + e)
                remote(
                    heads_own.at[fine(i), :],
                    h_slot(i, who),
                    h_send.at[k, i],
                    h_recv.at[slot, i],
                    "tp",
                    who,
                ).wait_recv()

    def e_copy(n, i, who):
        if n == 2:
            size = hidden_w // parts
            at = pl.ds(pl.multiple_of(i * size, size), size)
            dst = down_w.at[pl.ds(pl.multiple_of(who * hidden_w + i * size, size), size), :]
            src = down_hbm.at[at, :]
        else:
            size = full // parts
            at = pl.ds(pl.multiple_of(i * size, size), size)
            dst = (gate_w, up_w)[n].at[at, cols(who, hidden_w)]
            src = (gate_hbm, up_hbm)[n].at[at, :]
        return remote(src, dst, e_send.at[n, i], e_recv.at[n, i], "tp", pt)

    def share_weights(first, stop):
        for i in range(first, stop):
            for n in range(3):
                e_copy(n, i, c).start()

    def w_slot(who):
        return wo_full.at[cols(who, hw), :]

    def w_rows(k, j, b):
        start = from_tp(k) * hw + j * share + b * sub
        return wo_full.at[pl.ds(pl.multiple_of(start, sub), sub), :]

    def pair_rows(k, j, b):
        start = pair_tp(k) * hw + j * share + b * sub
        return wo_full.at[pl.ds(pl.multiple_of(start, sub), sub), :]

    def far_copy(k, b):
        src = wo_hbm.at[pl.ds(pl.multiple_of(r * share + b * sub, sub), sub), :]
        dst = wo_full.at[pl.ds(pl.multiple_of(t * hw + r * share + b * sub, sub), sub), :]
        return remote(src, dst, f_send.at[k - 1, b], f_recv.at[k - 1, b], "tp", to_tp(k))

    def twin_copy(k, b):
        slot = w_rows(k, r, b)
        return remote(slot, slot, q_send.at[k - 1, b], q_recv.at[k - 1, b], "seq", twin)

    def pass_copy(k, g, j, b):
        slot = w_rows(k, j, b)
        return remote(slot, slot, b_send.at[k - 1, g, b], b_recv.at[k - 1, g, b], "tp", pt)

    def spread(b):
        for k in range(1, half):
            far_copy(k, b).wait_recv()
            if group > 1:
                twin_copy(k, b).start()
            pass_copy(k, 0, r, b).start()

    def spread_twin(b):
        for k in range(1, half):
            if group > 1:
                twin_copy(k, b).wait_recv()
                pass_copy(k, 1, 1 - r, b).start()

    def w_copy(slot, src, who, other):
        return remote(src, w_slot(who), w_send.at[slot], w_recv.at[slot], "tp", other)

    def send_x(i, carry):
        for k in range(1, half):
            x_copy(k, i, x_slot(i, t), t, to_tp(k)).start()
        x_copy(0, i, x_slot(i, t), t, pt).start()
        return carry

    lax.fori_loop(0, nc, send_x, 0)
    for load in loads[2:]:
        load.start()
    w_copy(0, wo_hbm, t, pt).start()
    share_weights(0, parts // 2)
    for load in small:
        load.wait()

    row_id = lax.broadcasted_iota(jnp.int32, (width, width), 0)
    col_id = lax.broadcasted_iota(jnp.int32, (width, width), 1)
    eye = (row_id == col_id).astype(f32)
    upto = (row_id <= col_id).astype(f32)
    for h in range(heads):
        state[h] = jnp.concatenate([eye, jnp.zeros((width, width), f32)], axis=1)

    xor = row_id ^ col_id

    def fold_gain(i, carry):
        at = cols(i, width)
        gain = jnp.broadcast_to(again_ref[:, at], (width, width)).T
        gain = jnp.concatenate([gain] * heads, axis=1)
        for j in range(3):
            qkv_w[j, at, :] = (qkv_w[j, at, :].astype(f32) * gain).astype(bf16)
        return carry

    def prepare(i, carry):
        at = fine(i)
        lanes = cols(i, width)
        cumul = jnp.dot(
            decay_ref[:, lanes], upto, precision=lax.Precision.HIGHEST, preferred_element_type=f32
        )
        rate = rate_ref[:, lanes]
        for h in range(heads):
            c_row = jnp.broadcast_to(cumul[h : h + 1, :], (width, width))
            c_col = c_row.T
            b_col = jnp.broadcast_to(rate[h : h + 1, :], (width, width)).T
            c_end = cumul[h : h + 1, width - 1 : width]
            weights = jnp.exp(jnp.minimum(c_col - c_row, 0.0))
            growth = jnp.exp(c_col)
            below_buf[h, at, :] = jnp.where(row_id > col_id, b_col * weights, 0.0)
            upto_buf[h, at, :] = jnp.where(row_id >= col_id, weights, 0.0)
            rate_buf[h, at, :] = b_col
            growth_buf[h, at, :] = growth
            grown_buf[h, at, :] = b_col * growth
            tail_buf[h, at, :] = jnp.exp(c_end - c_col)
            last_buf[i, h : h + 1, :] = jnp.broadcast_to(jnp.exp(c_end), (1, 2 * width))
        return carry

    lax.fori_loop(0, nh, prepare, 0)
    loads[1].wait()
    lax.fori_loop(0, full // width, fold_gain, 0)

    def gather(i):
        for k in range(1, half):
            x_copy(k, i, x_slot(i, from_tp(k)), from_tp(k), pt).wait_recv()
            x_copy(half - 1 + k, i, x_slot(i, from_tp(k)), from_tp(k), pt).start()

    def gathered(i):
        for k in range(1, half):
            x_copy(half - 1 + k, i, x_slot(i, pair_tp(k)), pair_tp(k), pt).wait_recv()

    def solve(lower, right):
        chains = list(lower)
        inverse = {cell: eye - jnp.where(xor < 2, lower[cell], 0.0) for cell in chains}
        block = 2
        while block < width:
            merge = 4 if 4 * block <= width else 2
            now = (xor >= block) & (xor < merge * block)
            small = {cell: inverse[cell].astype(bf16) for cell in chains}
            off = {
                cell: mm(small[cell], jnp.where(now, lower[cell], 0.0).astype(bf16)).astype(bf16)
                for cell in chains
            }
            block *= merge
            if block == width:
                inverse = {cell: mm(small[cell], right[cell]) for cell in chains}
                small = {cell: inverse[cell].astype(bf16) for cell in chains}
            inverse = {cell: inverse[cell] - mm(off[cell], small[cell]) for cell in chains}
            if merge == 4:
                square = {cell: mm(off[cell], off[cell]).astype(bf16) for cell in chains}
                inverse = {
                    cell: inverse[cell] + mm(square[cell], inverse[cell].astype(bf16))
                    for cell in chains
                }
        return inverse

    def chunk(first, subs, between=None):
        span = subs * width
        here = pl.ds(pl.multiple_of(first, width), span)
        square = square_buf[here, :1]
        q_all, k_all, v_all = [early_buf[n, here, :] for n in range(3)]
        for n in range(1, half):
            at = cols(pair_tp(n), cw)
            x = x_full[here, at]
            wide = x.astype(f32)
            square = square + jnp.sum(wide * wide, axis=1, keepdims=True)
            k_all = k_all + mm(x, qkv_w[1, at, :])
            v_all = v_all + mm(x, qkv_w[2, at, :])
            q_all = q_all + mm(x, qkv_w[0, at, :])
        scale = lax.rsqrt(square * (1.0 / full) + norm_floor)
        q_all, k_all, v_all = q_all * scale, k_all * scale, v_all * scale
        chains = [(c, h) for c in range(subs) for h in range(heads)]
        lower, mixing, right, tail, growth_q, last = {}, {}, {}, {}, {}, {}
        for c in range(subs):
            at = pl.ds(pl.multiple_of(first + c * width, width), width)
            for h in range(heads):
                cell = (c, h)
                part = (slice(c * width, (c + 1) * width), slice(h * width, (h + 1) * width))
                q = unit_rows(q_all[part])
                k = unit_rows(k_all[part])
                kb = k.astype(bf16)
                both = mm_nt(jnp.concatenate([kb, q.astype(bf16)], axis=0), kb)
                lower[cell] = both[:width] * below_buf[h, at, :]
                mixing[cell] = (both[width:] * upto_buf[h, at, :]).astype(bf16)
                right[cell] = jnp.concatenate(
                    [rate_buf[h, at, :] * v_all[part], grown_buf[h, at, :] * k], axis=1
                ).astype(bf16)
                tail[cell] = (k * tail_buf[h, at, :]).astype(bf16)
                growth_q[cell] = growth_buf[h, at, :] * q
                last[cell] = last_buf[first // width + c, h : h + 1, :]
        answer = solve(lower, right)
        solved = {cell: answer[cell].astype(bf16) for cell in chains}
        moved = {cell: mm_tn(tail[cell], solved[cell]) for cell in chains}
        before_b = {}
        for c in range(subs):
            for h in range(heads):
                cell = (c, h)
                before = state[h]
                before_b[cell] = before.astype(bf16)
                change = mm(moved[cell][:, width:].astype(bf16), before_b[cell])
                after = last[cell] * before - change
                state[h] = jnp.concatenate(
                    [after[:, :width], after[:, width:] + moved[cell][:, :width]], axis=1
                )
        if between is not None:
            between()
        mixed = {cell: mm(mixing[cell], solved[cell]) for cell in chains}
        for c in range(subs):
            at = pl.ds(pl.multiple_of(first + c * width, width), width)
            for h in range(heads):
                cell = (c, h)
                lanes = slice(h * width, (h + 1) * width)
                entry = (growth_q[cell] - mixed[cell][:, width:]).astype(bf16)
                entered = mm(entry, before_b[cell])
                p_buf[at, lanes] = entered[:, :width].astype(bf16)
                o_buf[at, lanes] = mixed[cell][:, :width] + entered[:, width:]

    def s_copy(j, h):
        src, dst = (s_send_buf.at[j, h], s_recv_buf.at[j, h])
        if j + 1 == steps:
            src, dst = (last_send_buf.at[h], last_recv_buf.at[h])
        return remote(src, dst, s_send.at[j, h], s_recv.at[j, h], "seq", lax.rem(s + 2**j, n_seq))

    def s_start(j, h):
        @pl.when(s + 2**j < n_seq)
        def _():
            if j + 1 == steps:
                last_send_buf[h] = state[h, :, width:].astype(bf16)
            else:
                s_send_buf[j, h] = state[h].astype(bf16)
            s_copy(j, h).start()

    early = [[] for _ in range(steps)]
    early_twin = [[] for _ in range(steps)]
    for b, j in enumerate(EARLY[:nb]):
        if j < steps:
            early[j].append(b)
    for b, j in enumerate(EARLY_TWIN[:nb]):
        if j < steps:
            early_twin[j].append(b)

    subs = 2 if nh % 2 == 0 else 1
    per = subs * width // span
    big = nh // subs

    def stage_one(i, carry):
        for n in range(1, per):
            gather(per * i + n)

        @pl.when(i == FAR)
        def _():
            for b in range(nb):
                for k in range(1, half):
                    far_copy(k, b).start()
            share_weights(parts // 2, parts)

        here = pl.ds(pl.multiple_of(i * subs * width, subs * width), subs * width)
        for k in range(1, half):
            at = cols(from_tp(k), cw)
            x = x_full[here, at]
            wide = x.astype(f32)
            square_buf[here, :] += jnp.broadcast_to(
                jnp.sum(wide * wide, axis=1, keepdims=True), (subs * width, width)
            )
            for n in range(3):
                early_buf[n, here, :] += mm(x, qkv_w[n, at, :])
        for n in range(per):
            gathered(per * i + n)

        def between():
            @pl.when(i + 1 < big)
            def _():
                gather(per * (i + 1))

            @pl.when(i + 1 == big)
            def _():
                for h in range(heads):
                    excl[h] = jnp.concatenate([eye, jnp.zeros((width, width), f32)], axis=1)
                    if steps > 0:
                        s_start(0, h)

        chunk(i * subs * width, subs, between)
        return carry

    def stage_zero(i, carry):
        for n in range(per):
            x_copy(0, per * i + n, x_slot(per * i + n, pt), pt, pt).wait_recv()
        at = cols(chip, 2 * cw)
        here = pl.ds(pl.multiple_of(i * subs * width, subs * width), subs * width)
        x = x_full[here, at]
        wide = x.astype(f32)
        square = jnp.sum(wide * wide, axis=1, keepdims=True)
        square_buf[here, :] = jnp.broadcast_to(square, (subs * width, width))
        for n in range(3):
            early_buf[n, here, :] = mm(x, qkv_w[n, at, :])
        return carry

    lax.fori_loop(0, big, stage_zero, 0)
    gather(0)
    lax.fori_loop(0, big, stage_one, 0)
    for j in range(steps):
        for b in early[j]:
            spread(b)
        for b in early_twin[j]:
            spread_twin(b)
        for h in range(heads):

            @pl.when(s >= 2**j)
            def _(j=j, h=h):
                s_copy(j, h).wait_recv()
                if j + 1 == steps:
                    mine = excl[h]
                    got = last_recv_buf[h]
                    excl[h, :, width:] = split_mm(mine[:, :width], got) + mine[:, width:]
                    return
                got = s_recv_buf[j, h]
                mine = state[h]
                new = split_mm(mine[:, :width], got)
                state[h] = jnp.concatenate(
                    [new[:, :width], new[:, width:] + mine[:, width:]], axis=1
                )

            if j + 1 < steps:
                s_start(j + 1, h)

                @pl.when(s >= 2**j)
                def _(j=j, h=h):
                    got = s_recv_buf[j, h]
                    if j == 0:
                        excl[h] = got.astype(f32)
                        return
                    mine = excl[h]
                    new = split_mm(mine[:, :width], got)
                    excl[h] = jnp.concatenate(
                        [new[:, :width], new[:, width:] + mine[:, width:]], axis=1
                    )

    def stage_two(i, carry):
        for h in range(heads):
            lanes = slice(h * width, (h + 1) * width)
            start = excl[h, :, width:].astype(bf16)
            raw = o_buf[fine(i), lanes] + mm(p_buf[fine(i), lanes], start)
            scale = lax.rsqrt(jnp.mean(raw * raw, axis=1, keepdims=True) + head_floor)
            heads_own[fine(i), lanes] = (raw * scale * hgain_ref[...]).astype(bf16)
        for k in range(1, half):
            h_copy(k, i).start()

        @pl.when(lax.rem(i, 2) != c)
        def _():
            h_copy(0, i).start()

        @pl.when(lax.rem(i, 2) == c)
        def _():
            heads_all[fine(i // 2), cols(t, hw)] = heads_own[fine(i), :]

        return carry

    lax.fori_loop(0, nh, stage_two, 0)
    loads[2].wait()
    w_copy(0, w_slot(pt), pt, pt).wait_recv()

    def own_part(i, carry):
        h_wait(i, range(1))
        at = cols(chip, 2 * hw)
        x = x_full[fine(2 * i + c), :].astype(f32)
        own_buf[fine(i), :] = x + mm(heads_all[fine(i), at], wo_full[at, :])
        return carry

    lax.fori_loop(0, mine, own_part, 0)
    for b in range(nb):
        if not any(b in some for some in early):
            spread(b)
    for b in range(nb):
        if not any(b in some for some in early_twin):
            spread_twin(b)
    for load in loads[3:]:
        load.wait()
    for i in range(parts):
        for n in range(3):
            e_copy(n, i, 1 - c).wait_recv()

    def base_copy(i):
        return remote(
            pair_buf.at[fine(i), :],
            base_buf.at[fine(2 * i + c), :],
            rp_send.at[i],
            rp_recv.at[i],
            "tp",
            pt,
        )

    def rc_copy(k, e, i):
        p = 2 * i + c
        return remote(
            part_buf.at[fine(i), cols(cross(k, e), cw)],
            cr_buf.at[k - 1, fine(p), :],
            rc_send.at[k - 1, e, i],
            rc_recv.at[k - 1, p],
            "tp",
            cross(k, e),
        )


    for k in range(1, half):
        for b in range(nb):
            for g in range(group):
                slot = pair_rows(k, r + g * (1 - 2 * r), b)
                remote(
                    slot, slot, b_send.at[k - 1, g, b], b_recv.at[k - 1, g, b], "tp", pt
                ).wait_recv()

    def stage_three(i, carry):
        p = 2 * i + c
        h_wait(i, range(1, half))
        res = own_buf[fine(i), :]
        for n in range(1, half):
            at = cols(lax.rem(chip + n, half), 2 * hw)
            res = res + mm(heads_all[fine(i), at], wo_full[at, :])
        scale = lax.rsqrt(jnp.mean(res * res, axis=1, keepdims=True) + norm_floor)
        res_tmp[...] = res
        normed = (res * scale * fgain_ref[...]).astype(bf16)
        gate = mm(normed, gate_w[...])
        up = mm(normed, up_w[...])
        hidden = (gate / (1.0 + jnp.exp(-gate)) * up).astype(bf16)
        part = mm(hidden, down_w[...])
        part_buf[fine(i), :] = part.astype(bf16)
        for k in range(1, half):
            for e in range(2):
                rc_copy(k, e, i).start()
        res_tmp[...] = res_tmp[...] + part
        pair_buf[fine(i), :] = res_tmp[:, cols(pt, cw)]
        base_copy(i).start()
        base_buf[fine(p), :] = res_tmp[:, cols(t, cw)]
        return carry

    lax.fori_loop(0, mine, stage_three, 0)

    def finish(p, carry):
        @pl.when(lax.rem(p, 2) != c)
        def _():
            remote(
                pair_buf.at[fine(p // 2), :],
                base_buf.at[fine(p), :],
                rp_send.at[p // 2],
                rp_recv.at[p // 2],
                "tp",
                pt,
            ).wait_recv()

        total = base_buf[fine(p), :]
        for k in range(1, half):
            remote(
                part_buf.at[fine(p // 2), cols(t, cw)],
                cr_buf.at[k - 1, fine(p), :],
                rc_send.at[k - 1, 0, p // 2],
                rc_recv.at[k - 1, p],
                "tp",
                crossed(k, lax.rem(p, 2)),
            ).wait_recv()
            total = total + cr_buf[k - 1, fine(p), :].astype(f32)
        out_ref[fine(p), :] = total.astype(bf16)
        return carry

    lax.fori_loop(0, nh, finish, 0)

    def drain(i, carry):
        for k in range(1, half):
            x_copy(k, i, x_slot(i, t), t, to_tp(k)).wait_send()
            x_copy(half - 1 + k, i, x_slot(i, from_tp(k)), from_tp(k), pt).wait_send()
        x_copy(0, i, x_slot(i, t), t, pt).wait_send()
        return carry

    def drain_heads(i, carry):
        for k in range(1, half):
            h_copy(k, i).wait_send()

        @pl.when(lax.rem(i, 2) != c)
        def _():
            h_copy(0, i).wait_send()

        return carry

    def drain_fine(i, carry):
        for k in range(1, half):
            for e in range(2):
                rc_copy(k, e, i).wait_send()
        base_copy(i).wait_send()
        return carry

    lax.fori_loop(0, nc, drain, 0)
    lax.fori_loop(0, nh, drain_heads, 0)
    lax.fori_loop(0, mine, drain_fine, 0)
    for i in range(parts):
        for n in range(3):
            e_copy(n, i, c).wait_send()
    for k in range(1, half):
        for b in range(nb):
            far_copy(k, b).wait_send()
            if group > 1:
                twin_copy(k, b).wait_send()
            for g in range(group):
                pass_copy(k, g, r + g * (1 - 2 * r), b).wait_send()
    w_copy(0, wo_hbm, t, pt).wait_send()
    for j in range(steps):

        @pl.when(s + 2**j < n_seq)
        def _(j=j):
            for h in range(heads):
                s_copy(j, h).wait_send()


def body(n_tp, n_seq, x, again, qkv, decay, rate, hgain, wo, fgain, gate, up, down):
    length, cw = x.shape
    width = hgain.shape[0]
    heads = qkv.shape[2] // width
    hw = heads * width
    full = cw * n_tp
    parts = 4
    half = n_tp // 2
    span = XG * width
    nc = length // span
    steps = (n_seq - 1).bit_length()
    slots = 2 * half - 1
    nh = length // width
    group = 2 if n_seq % 2 == 0 else 1
    nb = 4
    anywhere = pl.BlockSpec(memory_space=pl.ANY)
    dma = pltpu.SemaphoreType.DMA
    return pl.pallas_call(
        functools.partial(kernel, (n_tp, n_seq, span, width, steps, group, nb)),
        out_shape=pltpu.VMEM((length, cw), bf16),
        in_specs=[anywhere] * 11,
        out_specs=pl.BlockSpec(memory_space=pltpu.VMEM),
        scratch_shapes=[
            pltpu.VMEM((1, full), f32),
            pltpu.VMEM(decay.shape, f32),
            pltpu.VMEM(rate.shape, f32),
            pltpu.VMEM((1, width), f32),
            pltpu.VMEM((1, full), f32),
            *[pltpu.VMEM((heads, length, width), f32)] * 6,
            pltpu.VMEM((nh, heads, 2 * width), f32),
            pltpu.VMEM((3, length, hw), f32),
            pltpu.VMEM((length, width), f32),
            pltpu.VMEM((length // 2, full), f32),
            pltpu.VMEM((length, full), bf16),
            pltpu.VMEM(qkv.shape, bf16),
            pltpu.VMEM((full, 2 * gate.shape[1]), bf16),
            pltpu.VMEM((full, 2 * up.shape[1]), bf16),
            pltpu.VMEM((2 * down.shape[0], full), bf16),
            pltpu.VMEM((hw * n_tp, full), bf16),
            pltpu.VMEM((length, hw), f32),
            pltpu.VMEM((length, hw), bf16),
            pltpu.VMEM((length // 2, hw * n_tp), bf16),
            pltpu.VMEM((heads, width, 2 * width), f32),
            pltpu.VMEM((heads, width, 2 * width), f32),
            pltpu.VMEM((steps, heads, width, 2 * width), bf16),
            pltpu.VMEM((steps, heads, width, 2 * width), bf16),
            pltpu.VMEM((heads, width, width), bf16),
            pltpu.VMEM((heads, width, width), bf16),
            pltpu.VMEM((length, hw), bf16),
            pltpu.VMEM((width, full), f32),
            pltpu.VMEM((length, cw), f32),
            pltpu.VMEM((length // 2, cw), f32),
            pltpu.VMEM((length // 2, full), bf16),
            pltpu.VMEM((half - 1, length, cw), bf16),
            dma((11,)),
            dma((slots, nc)),
            dma((slots, nc)),
            dma((1,)),
            dma((1,)),
            dma((half - 1, nb)),
            dma((half - 1, nb)),
            dma((half - 1, nb)),
            dma((half - 1, nb)),
            dma((half - 1, group, nb)),
            dma((half - 1, group, nb)),
            dma((half, nh)),
            dma((slots, nh // 2)),
            dma((steps, heads)),
            dma((steps, heads)),
            dma((3, parts)),
            dma((3, parts)),
            dma((nh // 2,)),
            dma((nh // 2,)),
            dma((half - 1, 2, nh // 2)),
            dma((half - 1, nh)),
        ],
        compiler_params=pltpu.CompilerParams(
            collective_id=0, has_side_effects=True, vmem_limit_bytes=VL * 1024 * 1024
        ),
    )(
        x,
        again.reshape(1, full),
        qkv,
        decay,
        rate,
        hgain.reshape(1, width),
        wo,
        fgain.reshape(1, full),
        gate,
        up,
        down,
    )


def solution(mesh):
    placed = (
        P("seq", "tp"),
        P(),
        P(None, None, "tp"),
        P("tp", "seq"),
        P("tp", "seq"),
        P(),
        P("tp", None),
        P(),
        P(None, "tp"),
        P(None, "tp"),
        P("tp", None),
    )
    return jax.shard_map(
        functools.partial(body, mesh.shape["tp"], mesh.shape["seq"]),
        mesh=mesh,
        in_specs=placed,
        out_specs=P("seq", "tp"),
        check_vma=False,
    )
```
